32 devices in a mesh: dp: 2 (over x), ch: 4 (over z), wd: 4 (over y, core).
Axes of the slice: x: 2, y: 2, z: 4, core: 2. Of those that a mesh axis runs over, the one named last changes fastest.
Arguments:
- resid_in: bfloat16 [8192, 4096], P('dp', 'wd'), parts along dimension 0
- seg_pos: int32 [2, 4096], P('dp'), parts along dimension 0
- gain_temporal: bfloat16 [4096], P('wd')
- w_x: bfloat16 [4096, 4096], P('wd', 'ch')
- bias_x: bfloat16 [4096], P('ch')
- w_y: bfloat16 [4096, 4096], P('wd', 'ch')
- bias_y: bfloat16 [4096], P('ch')
- conv_w: bfloat16 [4, 4096], P(None, 'ch')
- conv_bias: bfloat16 [4096], P('ch')
- lam_param: float32 [4096], P('ch')
- rgate_w: bfloat16 [16, 256, 256], P('ch')
- rgate_b: bfloat16 [4096], P('ch')
- igate_w: bfloat16 [16, 256, 256], P('ch')
- igate_b: bfloat16 [4096], P('ch')
- w_o: bfloat16 [4096, 4096], P('ch', 'wd')
- bias_o: bfloat16 [4096], P('wd')
- gain_mlp: bfloat16 [4096], P('wd')
- w_g: bfloat16 [4096, 12288], P('wd', 'ch')
- bias_g: bfloat16 [12288], P('ch')
- w_u: bfloat16 [4096, 12288], P('wd', 'ch')
- bias_u: bfloat16 [12288], P('ch')
- w_d: bfloat16 [12288, 4096], P('ch', 'wd')
- bias_d: bfloat16 [4096], P('wd')
Outputs:
- output: bfloat16 [8192, 4096], P('dp', 'wd'), parts along dimension 0
There are 2 independent parts. The reference program is written for one: setup_inputs(seed, part) draws one part's arguments, and reference() takes and returns one part's arrays. A program takes and returns all parts, laid end to end along the dimension named above; an argument that names none is the same for every part.
All inputs are finite; a program needn't handle non-finite values.
Results may differ from the reference program's by a relative error of at most 0.0129929.
Values are sent between devices in bfloat16 or wider.
A program may use at most 1 GiB of HBM per device.

```python
import jax
import jax.numpy as jnp
from jax import lax

D = 4096
D_RNN = 4096
F = 12288
BLOCKS = 16
B = 1
T = 4096
CONV_WIDTH = 4
BLOCK_WIDTH = D_RNN // BLOCKS
EPS = 1e-6


def normal_draw(key, shape, scale):
    return (jax.random.normal(key, shape, jnp.float32) * scale).astype(jnp.bfloat16)


def doc_positions(key):
    cuts = jax.random.randint(key, (B, 4), 0, T)
    steps = jnp.arange(T, dtype=jnp.int32)
    starts = jnp.any(steps[None, :, None] == cuts[:, None, :], axis=2) | (steps == 0)[None, :]
    last_start = lax.cummax(jnp.where(starts, steps[None, :], 0), axis=1)
    return (steps[None, :] - last_start).astype(jnp.int32)


def setup_inputs(seed: int = 0, part: int = 0) -> dict:
    root = jax.random.key(seed)
    part_key = jax.random.fold_in(root, part)
    keys = jax.random.split(root, 24)
    col_ramp = 0.5 + 1.5 * jnp.arange(D, dtype=jnp.float32) / D
    noise = jax.random.normal(jax.random.fold_in(part_key, 0), (B * T, D), jnp.float32)
    decay_target = jax.random.uniform(keys[9], (D_RNN,), jnp.float32, 0.9, 0.999)
    sigma_lam = decay_target ** 0.125
    return {
        'resid_in': (noise * col_ramp).astype(jnp.bfloat16),
        'seg_pos': doc_positions(jax.random.fold_in(part_key, 1)),
        'gain_temporal': normal_draw(keys[0], (D,), 0.5),
        'w_x': normal_draw(keys[1], (D, D_RNN), D ** -0.5),
        'bias_x': normal_draw(keys[2], (D_RNN,), 0.5),
        'w_y': normal_draw(keys[3], (D, D_RNN), D ** -0.5),
        'bias_y': normal_draw(keys[4], (D_RNN,), 0.5),
        'conv_w': normal_draw(keys[5], (CONV_WIDTH, D_RNN), 0.5),
        'conv_bias': normal_draw(keys[6], (D_RNN,), 0.5),
        'lam_param': jnp.log(sigma_lam / (1.0 - sigma_lam)),
        'rgate_w': normal_draw(keys[7], (BLOCKS, BLOCK_WIDTH, BLOCK_WIDTH), BLOCK_WIDTH ** -0.5),
        'rgate_b': normal_draw(keys[8], (D_RNN,), 1.0),
        'igate_w': normal_draw(keys[10], (BLOCKS, BLOCK_WIDTH, BLOCK_WIDTH), BLOCK_WIDTH ** -0.5),
        'igate_b': normal_draw(keys[11], (D_RNN,), 1.0),
        'w_o': normal_draw(keys[12], (D_RNN, D), 1.5 * D_RNN ** -0.5),
        'bias_o': normal_draw(keys[13], (D,), 0.5),
        'gain_mlp': normal_draw(keys[14], (D,), 0.5),
        'w_g': normal_draw(keys[15], (D, F), D ** -0.5),
        'bias_g': normal_draw(keys[16], (F,), 0.5),
        'w_u': normal_draw(keys[17], (D, F), D ** -0.5),
        'bias_u': normal_draw(keys[18], (F,), 0.5),
        'w_d': normal_draw(keys[19], (F, D), 1.5 * F ** -0.5),
        'bias_d': normal_draw(keys[20], (D,), 0.5),
    }


def rms_scale(vals, gain):
    mean_sq = jnp.mean(vals * vals, axis=-1, keepdims=True)
    return (vals * lax.rsqrt(mean_sq + EPS) * (1.0 + gain.astype(jnp.float32))).astype(jnp.bfloat16)


def conv_mix(vals, positions, conv_w, conv_bias):
    vals32 = vals.astype(jnp.float32)
    taps = conv_w.astype(jnp.float32)
    total = conv_bias.astype(jnp.float32) + vals32 * taps[0]
    for shift in range(1, CONV_WIDTH):
        moved = jnp.pad(vals32[:-shift], ((shift, 0), (0, 0)))
        total = total + jnp.where((positions >= shift)[:, None], moved, 0.0) * taps[shift]
    return total.astype(jnp.bfloat16)


def combine(left, right):
    return left[0] * right[0], right[0] * left[1] + right[1]


def rg_lru(conv_out, positions, lam_param, rgate_w, rgate_b, igate_w, igate_b):
    grouped = conv_out.astype(jnp.float32).reshape(T, BLOCKS, BLOCK_WIDTH)
    rate = jax.nn.sigmoid(jnp.einsum('tbi,bij->tbj', grouped, rgate_w.astype(jnp.float32)).reshape(T, D_RNN) + rgate_b.astype(jnp.float32))
    inflow = jax.nn.sigmoid(jnp.einsum('tbi,bij->tbj', grouped, igate_w.astype(jnp.float32)).reshape(T, D_RNN) + igate_b.astype(jnp.float32))
    log_a = -8.0 * rate * jax.nn.softplus(-lam_param.astype(jnp.float32))
    reset = (positions == 0)[:, None]
    decay = jnp.where(reset, 0.0, jnp.exp(log_a))
    scale = jnp.where(reset, 1.0, jnp.sqrt(-jnp.expm1(2.0 * log_a)))
    drive = scale * inflow * conv_out.astype(jnp.float32)
    return lax.associative_scan(combine, (decay, drive), axis=0)[1]


def reference(resid_in, seg_pos, gain_temporal, w_x, bias_x, w_y, bias_y, conv_w, conv_bias, lam_param, rgate_w, rgate_b, igate_w, igate_b, w_o, bias_o, gain_mlp, w_g, bias_g, w_u, bias_u, w_d, bias_d):
    def one_sequence(pair):
        seq_x, positions = pair
        resid32 = seq_x.astype(jnp.float32)
        normed = rms_scale(resid32, gain_temporal)
        y_branch = jax.nn.gelu(jnp.dot(normed, w_y, preferred_element_type=jnp.float32) + bias_y.astype(jnp.float32), approximate=True).astype(jnp.bfloat16)
        u_branch = (jnp.dot(normed, w_x, preferred_element_type=jnp.float32) + bias_x.astype(jnp.float32)).astype(jnp.bfloat16)
        conv_out = conv_mix(u_branch, positions, conv_w, conv_bias)
        hidden = rg_lru(conv_out, positions, lam_param, rgate_w, rgate_b, igate_w, igate_b)
        mixed = (hidden * y_branch.astype(jnp.float32)).astype(jnp.bfloat16)
        resid = resid32 + jnp.dot(mixed, w_o, preferred_element_type=jnp.float32) + bias_o.astype(jnp.float32)
        normed2 = rms_scale(resid, gain_mlp)
        gate = jax.nn.gelu(jnp.dot(normed2, w_g, preferred_element_type=jnp.float32) + bias_g.astype(jnp.float32), approximate=True)
        upper = jnp.dot(normed2, w_u, preferred_element_type=jnp.float32) + bias_u.astype(jnp.float32)
        inner = (gate * upper).astype(jnp.bfloat16)
        return (resid + jnp.dot(inner, w_d, preferred_element_type=jnp.float32) + bias_d.astype(jnp.float32)).astype(jnp.bfloat16)
    per_seq = lax.map(one_sequence, (resid_in.reshape(B, T, D), seg_pos))
    return per_seq.reshape(B * T, D)
```

```python
import functools

import jax
import jax.numpy as jnp
from jax import lax
from jax.experimental import pallas as pl
from jax.experimental.pallas import tpu as pltpu
from jax.sharding import PartitionSpec as P


EPS = 1e-6
CHUNKS = 2
SUB = 16
TILE = 256
PIECES = 4
GROUP = 8
WAYS = (0, 1)
BLOCKS = (0, 1, 2, 3)
OTHERS = BLOCKS[1:]
LIMIT = 60 * 2 ** 20
WORK = pl.CostEstimate(flops=2 * 10 ** 11, bytes_accessed=2 * 10 ** 7, transcendentals=0)
MESH = pl.DeviceIdType.MESH
F32 = jnp.float32
BF16 = jnp.bfloat16


def flip_pairs(count, r):
    return [(i, i ^ r) for i in range(count)]


def dot32(a, b):
    return jnp.dot(a, b, preferred_element_type=F32)


def lru_body(idx_ref, own_ref, peer_ref, far_ref, pos_ref, bias_ref, conv_ref, sp_ref, gate_w_ref, gate_b_ref, tail_ref, carry_ref, mixed_ref, tail_out, carry_out, ubuf, abuf, bbuf, carry):
    step = pl.program_id(0)
    rows, width = abuf.shape

    @pl.when(step == 0)
    def _():
        ubuf[:GROUP, :] = tail_ref[...]
        carry[...] = carry_ref[...]

    @pl.when(step > 0)
    def _():
        ubuf[:GROUP, :] = ubuf[rows:, :]

    total = own_ref[...].astype(F32) + peer_ref[...].astype(F32) + far_ref[...].astype(F32) + bias_ref[...]
    ubuf[GROUP:, :] = total[:, :width].astype(BF16).astype(F32)
    pos = pos_ref[...]
    conv = conv_ref[4:5, :] + ubuf[GROUP:, :] * conv_ref[0:1, :]
    for shift in OTHERS:
        moved = ubuf[GROUP - shift:rows + GROUP - shift, :]
        conv = conv + jnp.where(pos >= shift, moved, 0.0) * conv_ref[shift:shift + 1, :]
    conv_b = conv.astype(BF16)
    conv32 = conv_b.astype(F32)
    gates = jax.nn.sigmoid(dot32(conv_b, gate_w_ref[...]) + gate_b_ref[...])
    rate = gates[:, :width]
    inflow = gates[:, width:]
    depth = 8.0 * rate * sp_ref[...]
    twice = 2.0 * depth
    series = 1.0
    for k in (5, 4, 3, 2):
        series = 1.0 - (twice * series) / k
    series = twice * series
    left = jnp.where(twice < 0.125, series, 1.0 - jnp.exp(-twice))
    reset = pos == 0
    abuf[...] = jnp.where(reset, 0.0, jnp.exp(-depth))
    bbuf[...] = jnp.where(reset, 1.0, jnp.sqrt(left)) * inflow * conv32

    row = lax.broadcasted_iota(jnp.int32, (GROUP, width), 0)

    def group(g, held):
        at = pl.multiple_of(g * GROUP, GROUP)
        a = abuf[pl.ds(at, GROUP), :]
        b = bbuf[pl.ds(at, GROUP), :]
        for d in (1, 2, 4):
            keep = row >= d
            b = b + a * jnp.where(keep, pltpu.roll(b, d, 0), 0.0)
            a = a * jnp.where(keep, pltpu.roll(a, d, 0), 1.0)
        bbuf[pl.ds(at, GROUP), :] = b + a * held
        last_a = jnp.broadcast_to(a[GROUP - 1:, :], (GROUP, width))
        last_b = jnp.broadcast_to(b[GROUP - 1:, :], (GROUP, width))
        return last_b + last_a * held

    held = lax.fori_loop(0, rows // GROUP, group, carry[...], unroll=GROUP)
    carry[...] = held
    y_branch = jax.nn.gelu(total[:, width:], approximate=True).astype(BF16)
    mixed_ref[...] = (bbuf[...] * y_branch.astype(F32)).astype(BF16).reshape(mixed_ref.shape)
    tail_out[...] = ubuf[rows:, :]
    carry_out[...] = held


def lru(idx, own, peer, far, pos, bias, conv, sp, gate_w, gate_b, tail, carry, rows):
    tokens = own.shape[0]
    width = own.shape[1] // 2
    blocks = tokens // rows
    wide = pl.BlockSpec((rows, 2 * width), lambda s, idx: (s, 0))
    full = lambda arr: pl.BlockSpec(arr.shape, lambda s, idx: (0,) * arr.ndim)
    state = jax.ShapeDtypeStruct((GROUP, width), F32)
    return pl.pallas_call(
        lru_body,
        grid_spec=pltpu.PrefetchScalarGridSpec(
            num_scalar_prefetch=1,
            grid=(blocks,),
            in_specs=[wide, wide, wide, pl.BlockSpec((rows, 1), lambda s, idx: (s, 0))] + [full(v) for v in (bias, conv, sp, gate_w, gate_b, tail, carry)],
            out_specs=[pl.BlockSpec((1, 1, rows, width), lambda s, idx: ((s % 4) ^ idx[0], s // 4, 0, 0)), full(tail), full(carry)],
            scratch_shapes=[pltpu.VMEM((rows + GROUP, width), F32), pltpu.VMEM((rows, width), F32), pltpu.VMEM((rows, width), F32), pltpu.VMEM((GROUP, width), F32)],
        ),
        out_shape=[jax.ShapeDtypeStruct((4, blocks // 4, rows, width), BF16), state, state],
        compiler_params=pltpu.CompilerParams(dimension_semantics=("arbitrary",)),
        cost_estimate=pl.CostEstimate(flops=tokens * width * 4000, bytes_accessed=tokens * width * 20, transcendentals=tokens * width * 8),
        name="lru",
    )(idx, own, peer, far, pos, bias, conv, sp, gate_w, gate_b, tail, carry)


def pieces_specs(pieces, cols):
    return [pl.BlockSpec((w.shape[0], cols), lambda j, idx: (0, j)) for w in pieces]


def put_rows(out_ref, r, val):
    zs, steps, _, rows, cols = out_ref.shape
    out_ref[:, :, r] = val.astype(BF16).reshape(zs, steps, rows, cols)


def down_body(idx_ref, inner_ref, own, core, far_a, far_b, both_a, both_b, out_ref):
    dp = idx_ref[1]
    half = inner_ref.shape[2]
    put = functools.partial(put_rows, out_ref)
    for r, w in ((0, own), (1, core)):
        put(r, dot32(inner_ref[0], w[0:half, :]) + dot32(inner_ref[1], w[half:2 * half, :]))
    for r, near, far in ((2, far_a, far_b), (3, both_a, both_b)):
        put(r, dot32(inner_ref[dp], near[...]) + dot32(inner_ref[1 - dp], far[...]))


def partial_rows(body, idx, lhs, pieces, grid_rows, cols):
    zs, steps, rows = grid_rows
    depth, width = pieces[0].shape
    return pl.pallas_call(
        body,
        grid_spec=pltpu.PrefetchScalarGridSpec(
            num_scalar_prefetch=1,
            grid=(width // cols,),
            in_specs=[pl.BlockSpec(lhs.shape, lambda j, idx: (0,) * lhs.ndim)] + pieces_specs(pieces, cols),
            out_specs=pl.BlockSpec((zs, steps, 4, rows, cols), lambda j, idx: (0, 0, 0, 0, j)),
        ),
        out_shape=jax.ShapeDtypeStruct((zs, steps, 4, rows, width), BF16),
        compiler_params=pltpu.CompilerParams(dimension_semantics=("arbitrary",)),
        cost_estimate=pl.CostEstimate(flops=2 * zs * steps * rows * depth * 4 * width, bytes_accessed=depth * 4 * width * 2, transcendentals=0),
    )(idx, lhs, *pieces)


def gate_up_body(idx_ref, m_ref, *refs):
    dp = idx_ref[1]
    g_parts, u_parts, (bias_g, bias_u, inner_ref) = refs[:6], refs[6:12], refs[12:]
    zs, steps, _, rows, depth = m_ref.shape
    lhs = lambda k: m_ref[:, :, k].reshape(zs * steps * rows, depth)

    def product(parts):
        own, core, far_a, far_b, both_a, both_b = parts
        acc = dot32(lhs(0), own[0:depth, :]) + dot32(lhs(1), own[depth:2 * depth, :])
        acc = acc + dot32(lhs(2), core[0:depth, :]) + dot32(lhs(3), core[depth:2 * depth, :])
        acc = acc + dot32(lhs(4 + dp), far_a[...]) + dot32(lhs(5 - dp), far_b[...])
        return acc + dot32(lhs(6 + dp), both_a[...]) + dot32(lhs(7 - dp), both_b[...])

    gate = jax.nn.gelu(product(g_parts) + bias_g[...], approximate=True)
    inner_ref[0] = (gate * (product(u_parts) + bias_u[...])).astype(BF16)


def gate_up(idx, m, g_pieces, u_pieces, bias_g, bias_u, cols):
    zs, steps, ks, rows, depth = m.shape
    steps = steps // 2
    toks = zs * steps * rows
    width = g_pieces[0].shape[1]
    tiles = width // cols
    bias_spec = pl.BlockSpec((1, cols), lambda j, idx: (0, j))
    return pl.pallas_call(
        gate_up_body,
        grid_spec=pltpu.PrefetchScalarGridSpec(
            num_scalar_prefetch=1,
            grid=(tiles,),
            in_specs=[pl.BlockSpec((zs, steps, ks, rows, depth), lambda j, idx: (0,) * 5)] + pieces_specs(g_pieces, cols) + pieces_specs(u_pieces, cols) + [bias_spec, bias_spec],
            out_specs=pl.BlockSpec((1, toks, cols), lambda j, idx: (j // (tiles // 2), 0, j % (tiles // 2))),
        ),
        out_shape=jax.ShapeDtypeStruct((2, toks, width // 2), BF16),
        compiler_params=pltpu.CompilerParams(dimension_semantics=("arbitrary",)),
        cost_estimate=pl.CostEstimate(flops=4 * toks * ks * depth * width, bytes_accessed=4 * ks * depth * width, transcendentals=toks * width),
        name="gate_up",
    )(idx, m, *g_pieces, *u_pieces, bias_g, bias_u)


def line_body(kind, n_ship, *refs):
    if kind == "norm":
        x_rows, (bias, gain, mixed), mix_in, o_parts = refs[:4], refs[4:7], refs[7:11], refs[11:17]
        ship, refs = refs[17:17 + n_ship], refs[17 + n_ship:]
        res_ref, out = refs[:2]
        shipped, refs = refs[2:2 + 5 * n_ship], refs[2 + 5 * n_ship:]
        rbuf, obuf, send, recv, loc, w_send, w_recv, part, mixbuf, wo, a_send, a_recv, pre_sem = refs
    else:
        part_a, res_ref, bias, m_all, bias_g, bias_u = refs[:6]
        g_parts, u_parts, d_parts = refs[6:12], refs[12:18], refs[18:24]
        out, rbuf, obuf, send, recv, loc, a_send, a_recv, part, mbuf, inner, wbuf, pre_sem, tile_sem = refs[24:]
    n = rbuf.shape[1] + 1
    steps = rbuf.shape[2]
    z, me, dp = lax.axis_index('ch'), lax.axis_index('wd'), lax.axis_index('dp')
    lag = 0 if kind == "norm" else 1
    wd_to = lambda r: {'wd': me ^ r}
    peers = [wd_to(r) for r in OTHERS] + ([{'dp': 1 - dp}] if kind == "norm" else [])

    barrier = pltpu.get_barrier_semaphore()
    for peer in peers:
        pl.semaphore_signal(barrier, inc=1, device_id=peer, device_id_type=MESH)

    @pl.when(z > 0)
    def _():
        pl.semaphore_signal(barrier, inc=1, device_id={'ch': z - 1}, device_id_type=MESH)

    @pl.when(z < n - 1)
    def _():
        pl.semaphore_signal(barrier, inc=1, device_id={'ch': z + 1}, device_id_type=MESH)

    @pl.when((z > 0) & (z < n - 1))
    def _():
        pl.semaphore_wait(barrier, len(peers) + 2)

    @pl.when((z == 0) | (z == n - 1))
    def _():
        pl.semaphore_wait(barrier, len(peers) + 1)

    place = lambda way: z if way == 0 else n - 1 - z
    there = lambda way, p: p if way == 0 else n - 1 - p

    def hop(way, slot, s, src, dst):
        return pltpu.make_async_remote_copy(src_ref=src, dst_ref=dst, send_sem=send.at[way, slot, s], recv_sem=recv.at[way, slot, s], device_id={'ch': there(way, jnp.minimum(place(way) + 1, n - 1))}, device_id_type=MESH)

    def reduce_hop(way, h, s, first):
        src = part.at[there(way, place(way) + n - h), s] if first else rbuf.at[way, h - 2, s]
        return hop(way, h - 1, s, src, rbuf.at[way, h - 1, s])

    def reduce_wait(way, h, s):
        at = rbuf.at[way, h - 1, s]
        hop(way, h - 1, s, at, at).wait_recv()

    def block_at(o, s):
        return out.at[o, s] if kind == "norm" else out.at[o, :, s]

    def gather_hop(way, h, s):
        at = block_at(there(way, place(way) - (h - 1)), s)
        src = obuf.at[s] if kind == "norm" and h == 1 else at
        return hop(way, n - 2 + h, s, src, at)

    def local_copy(s):
        src, dst = (obuf.at[s], out.at[z, s]) if kind == "norm" else (obuf.at[s, me], out.at[z, me, s])
        return pltpu.make_async_copy(src, dst, loc.at[s])

    def swap(r, s):
        return pltpu.make_async_remote_copy(src_ref=obuf.at[s, me ^ r], dst_ref=out.at[z, me, s], send_sem=a_send.at[r - 1, s], recv_sem=a_recv.at[r - 1, s], device_id=wd_to(r), device_id_type=MESH)

    def swapped(r, s):
        return pltpu.make_async_remote_copy(src_ref=obuf.at[s, me ^ r], dst_ref=out.at[z, me ^ r, s], send_sem=a_send.at[r - 1, s], recv_sem=a_recv.at[r - 1, s], device_id=wd_to(r), device_id_type=MESH)

    def weight_copy(q, j):
        i, p = q // PIECES, q % PIECES
        far_a, core, both_a, far_b, both_b = shipped[5 * i:5 * i + 5]
        size = far_a.shape[0] // PIECES
        own_at, at = pl.ds((PIECES * dp + p) * size, size), pl.ds(p * size, size)
        if j == 4:
            src, dst = ship[i], core
        elif j == 0:
            src, dst = ship[i].at[own_at], far_a.at[at]
        else:
            src, dst = ((far_a, far_b), (far_a, both_a), (far_b, both_b))[j - 1]
            src, dst = src.at[at], dst.at[at]
        to = (wd_to(2), {'dp': 1 - dp}, wd_to(1), wd_to(1), wd_to(1))[j]
        return pltpu.make_async_remote_copy(src_ref=src, dst_ref=dst, send_sem=w_send.at[q, j], recv_sem=w_recv.at[q, j], device_id=to, device_id_type=MESH)

    def row_places(pieces):
        own, core, far_a, far_b, both_a, both_b = pieces
        size, part_size = own.shape[0], far_a.shape[0]
        return ((own, 0), (core, size), (far_a, 2 * size + dp * part_size), (far_b, 2 * size + (1 - dp) * part_size), (both_a, 3 * size + dp * part_size), (both_b, 3 * size + (1 - dp) * part_size))

    def mix_copy(r, landed):
        there_at = mixbuf.at[me ^ r if landed else me, pl.ds(n - mixed.shape[1], mixed.shape[1])]
        return pltpu.make_async_remote_copy(src_ref=mixed.at[r], dst_ref=there_at, send_sem=a_send.at[r - 1], recv_sem=a_recv.at[r - 1], device_id=wd_to(r), device_id_type=MESH)

    if kind == "norm":
        for r in OTHERS:
            mix_copy(r, False).start()
        jobs = [(mixed.at[0], mixbuf.at[me, pl.ds(n - mixed.shape[1], mixed.shape[1])])]
        jobs += [(src, mixbuf.at[me ^ r, pl.ds(0, src.shape[0])]) for r, src in enumerate(mix_in)]
        jobs += [(w, wo.at[pl.ds(to, w.shape[0])]) for w, to in row_places(o_parts)]
        loads = [pltpu.make_async_copy(src, dst, pre_sem.at[j]) for j, (src, dst) in enumerate(jobs)]
        for copy in loads:
            copy.start()
        for q in range(PIECES * n_ship):
            weight_copy(q, 0).start()
        for i in range(n_ship):
            weight_copy(PIECES * i, 4).start()

        def project(j, _):
            d, r = lax.div(j, 4), lax.rem(j, 4)
            depth = mixbuf.shape[3]
            acc = None
            for b in BLOCKS:
                at = pl.ds(pl.multiple_of((4 * r + b) * depth, depth), depth)
                val = dot32(mixbuf[b, d], wo[at, :])
                acc = val if acc is None else acc + val
            part[d, :, r] = acc.astype(BF16).reshape(steps, part.shape[3], part.shape[4])
            return 0

        for copy in loads:
            copy.wait()
        first = 4 * mix_in[0].shape[0]
        lax.fori_loop(0, first, project, 0)
        for r in OTHERS:
            mix_copy(r, True).wait_recv()
        lax.fori_loop(first, 4 * n, project, 0)

    half = steps // 2
    if kind != "norm":
        gates = inner.shape[1] // TILE
        per_block = part.shape[4] // TILE
        tiles = gates + 4 * per_block
        loads = [pltpu.make_async_copy(part_a, part.at[:, pl.ds(0, half)], pre_sem.at[0]), pltpu.make_async_copy(m_all.at[:, pl.ds(half, half)], mbuf, pre_sem.at[1])]

        def tile_copies(q, down_block):
            slot = lax.rem(q, 2)
            if down_block is None:
                at = pl.ds(pl.multiple_of(q * TILE, TILE), TILE)
                jobs = [(w, i, to) for i, pieces in enumerate((g_parts, u_parts)) for w, to in row_places(pieces)]
            else:
                at = pl.ds(pl.multiple_of(lax.rem(q - gates, per_block) * TILE, TILE), TILE)
                own, core, far_a, far_b, both_a, both_b = d_parts
                rows_a = dp * far_a.shape[0]
                rows_b = far_a.shape[0] - rows_a
                jobs = ([(own, 0, 0)], [(core, 0, 0)], [(far_a, 0, rows_a), (far_b, 0, rows_b)], [(both_a, 0, rows_a), (both_b, 0, rows_b)])[down_block]
            return [pltpu.make_async_copy(w.at[:, at], wbuf.at[slot, i, pl.ds(to, w.shape[0]), :], tile_sem.at[slot, j]) for j, (w, i, to) in enumerate(jobs)]

        def for_tile(q, act):
            @pl.when(q < gates)
            def _():
                for copy in tile_copies(q, None):
                    act(copy)

            for r in BLOCKS:
                @pl.when((q >= gates + r * per_block) & (q < gates + (r + 1) * per_block))
                def _(r=r):
                    for copy in tile_copies(q, r):
                        act(copy)

        def mlp_tile(q, _):
            for_tile(q, lambda copy: copy.wait())
            for_tile(q + 1, lambda copy: copy.start())
            slot = lax.rem(q, 2)
            toks = inner.shape[0]

            @pl.when(q < gates)
            def _():
                at = pl.ds(pl.multiple_of(q * TILE, TILE), TILE)
                sums = []
                for i in range(2):
                    acc = None
                    depth = mbuf.shape[4]
                    for k in range(mbuf.shape[2]):
                        val = dot32(mbuf[:, :, k].reshape(toks, depth), wbuf[slot, i, k * depth:(k + 1) * depth, :])
                        acc = val if acc is None else acc + val
                    sums.append(acc)
                gate = jax.nn.gelu(sums[0] + bias_g[:, at], approximate=True)
                inner[:, at] = (gate * (sums[1] + bias_u[:, at])).astype(BF16)

            @pl.when(q >= gates)
            def _():
                d = q - gates
                at = pl.ds(pl.multiple_of(lax.rem(d, per_block) * TILE, TILE), TILE)
                val = dot32(inner[...], wbuf[slot, 0, 0:inner.shape[1], :]).astype(BF16)
                part[:, pl.ds(half, half), lax.div(d, per_block), :, at] = val.reshape(n, half, part.shape[3], TILE)

            return 0

        for copy in loads:
            copy.start()
        for_tile(0 * z, lambda copy: copy.start())
        for copy in loads:
            copy.wait()

    def finish(s):
        for way in WAYS:
            p = place(way)

            @pl.when(p > 0)
            def _(way=way):
                reduce_wait(way, n - 1, s)

        total = 0.0
        for r in BLOCKS:
            val = part[z, s, r].astype(F32)
            val = val + jnp.where(z > 0, rbuf[0, n - 2, s, r].astype(F32), 0.0)
            val = val + jnp.where(z < n - 1, rbuf[1, n - 2, s, r].astype(F32), 0.0)
            if kind == "norm":
                val = x_rows[r][s].astype(F32) + val + bias[r]
                res_ref[s, r] = val
                total = total + jnp.sum(val * val, axis=1, keepdims=True)
            else:
                obuf[s, me ^ r] = (res_ref[s, r] + val + bias[r]).astype(BF16)
        if kind == "norm":
            width = res_ref.shape[3]
            scale = lax.rsqrt(total / (4 * width) + EPS)
            for r in BLOCKS:
                normed = (res_ref[s, r] * scale * (1.0 + gain[r])).astype(BF16)
                obuf[s, 2 * r] = normed[:, :width // 2]
                obuf[s, 2 * r + 1] = normed[:, width // 2:]
        else:
            for r in OTHERS:
                swap(r, s).start()
        local_copy(s).start()

    def step(t, _):
        for h in range(n, 0, -1):
            s = t - (n - 1) - lag - (h - 1)

            @pl.when((s >= 0) & (s < steps))
            def _(h=h, s=s):
                if h == 1 and kind != "norm":
                    for r in OTHERS:
                        swapped(r, s).wait_recv()
                    local_copy(s).wait()
                if h == 1 and kind == "norm":
                    finish(s)
                for way in WAYS:
                    p = place(way)
                    if h > 1:
                        @pl.when(p >= h - 1)
                        def _(way=way):
                            at = block_at(there(way, place(way) - (h - 1)), s)
                            hop(way, n - 3 + h, s, at, at).wait_recv()
                    if h < n:
                        @pl.when((p >= h - 1) & (p < n - 1))
                        def _(way=way):
                            gather_hop(way, h, s).start()

        if lag:
            s = t - (n - 1)

            @pl.when((s >= 0) & (s < steps))
            def _(s=s):
                finish(s)

        for h in range(n - 1, 0, -1):
            s = t - (h - 1)
            for way in WAYS:
                p = place(way)

                @pl.when((s >= 0) & (s < steps) & (p < h))
                def _(h=h, s=s, way=way, p=p):
                    if h > 1:
                        @pl.when(p > 0)
                        def _():
                            reduce_wait(way, h - 1, s)
                            mine = part[there(way, p + n - h), s].astype(F32)
                            rbuf[way, h - 2, s] = (rbuf[way, h - 2, s].astype(F32) + mine).astype(BF16)
                            reduce_hop(way, h, s, False).start()

                    @pl.when(p == 0)
                    def _():
                        reduce_hop(way, h, s, True).start()

        if kind != "norm":
            @pl.when(t < half)
            def _():
                lax.fori_loop(lax.div(t * tiles, half), lax.div((t + 1) * tiles, half), mlp_tile, 0)

        if kind == "norm":
            for q in range(PIECES * n_ship):
                @pl.when(t == (3 * q + 9) // 2)
                def _(q=q):
                    weight_copy(q, 0).wait_recv()
                    weight_copy(q, 1).start()
                    weight_copy(q, 2).start()

                @pl.when(t == (3 * q + 14) // 2)
                def _(q=q):
                    weight_copy(q, 1).wait_recv()
                    weight_copy(q, 3).start()
        return 0

    lax.fori_loop(0, steps + 2 * n, step, 0)

    def drain(s, _):
        for way in WAYS:
            p = place(way)
            for h in range(1, n):
                @pl.when(p < h)
                def _(way=way, h=h):
                    reduce_hop(way, h, s, True).wait_send()

                @pl.when((p >= h - 1) & (p < n - 1))
                def _(way=way, h=h):
                    gather_hop(way, h, s).wait_send()
        if kind == "norm":
            local_copy(s).wait()
        else:
            for r in OTHERS:
                swap(r, s).wait_send()
        return 0

    lax.fori_loop(0, steps, drain, 0)
    if kind == "norm":
        for q in range(PIECES * n_ship):
            weight_copy(q, 0).wait_send()
            weight_copy(q, 2).wait()
            weight_copy(q, 1).wait_send()
            weight_copy(q, 3).wait()
        for i in range(n_ship):
            weight_copy(PIECES * i, 4).wait()
        for r in OTHERS:
            mix_copy(r, False).wait_send()


VM = pl.BlockSpec(memory_space=pltpu.VMEM)
ANY = pl.BlockSpec(memory_space=pl.ANY)
DMA = pltpu.SemaphoreType.DMA


def line_scratch(n, steps, block, done):
    sems = (2, 2 * n - 2, steps)
    return [pltpu.VMEM((2, n - 1, steps) + block, BF16), pltpu.VMEM((steps,) + done, BF16), DMA(sems), DMA(sems), DMA((steps,))]


def residual_norm(n, xs, bias, gain, mixed, mix_in, o_parts, ship):
    steps, rows, width = xs[0].shape
    out_w = []
    for w in ship:
        half = jax.ShapeDtypeStruct((w.shape[0] // 2, w.shape[1]), BF16)
        out_w += [half, jax.ShapeDtypeStruct(w.shape, BF16), half, half, half]
    done = (8, rows, width // 2)
    far = [mixed, *mix_in, *o_parts, *ship]
    pieces = PIECES * len(ship)
    outs = pl.pallas_call(
        functools.partial(line_body, "norm", len(ship)),
        in_specs=[VM] * 6 + [ANY] * len(far),
        out_specs=[VM, ANY] + [ANY] * len(out_w),
        out_shape=[jax.ShapeDtypeStruct((steps, 4, rows, width), F32), jax.ShapeDtypeStruct((n, steps) + done, BF16)] + out_w,
        scratch_shapes=line_scratch(n, steps, (4, rows, width), done) + [
            DMA((pieces, 5)), DMA((pieces, 5)),
            pltpu.VMEM((n, steps, 4, rows, width), BF16),
            pltpu.VMEM((4, n) + mixed.shape[2:], BF16),
            pltpu.VMEM((4 * width, width), BF16),
            DMA((3,)), DMA((3,)), DMA((11,)),
        ],
        compiler_params=pltpu.CompilerParams(collective_id=0, has_side_effects=True, vmem_limit_bytes=LIMIT),
        cost_estimate=WORK,
        name="residual_norm",
    )(*xs, bias, gain, *far)
    return outs[0], outs[1], [outs[2 + 5 * i:7 + 5 * i] for i in range(len(ship))]


def finish_rows(n, part_a, res, bias, m_all, bias_g, bias_u, pieces):
    steps, _, rows, width = res.shape
    half = steps // 2
    inner_width = bias_g.shape[1]
    toks = n * half * rows
    return pl.pallas_call(
        functools.partial(line_body, "finish", 0),
        in_specs=[ANY, VM, VM, ANY, VM, VM] + [ANY] * len(pieces),
        out_specs=ANY,
        out_shape=jax.ShapeDtypeStruct((n, 4, steps, rows, width), BF16),
        scratch_shapes=line_scratch(n, steps, (4, rows, width), (4, rows, width)) + [
            DMA((3, steps)), DMA((3, steps)),
            pltpu.VMEM((n, steps, 4, rows, width), BF16),
            pltpu.VMEM((n, half) + m_all.shape[2:], BF16),
            pltpu.VMEM((toks, inner_width), BF16),
            pltpu.VMEM((2, 2, 4 * width, TILE), BF16),
            DMA((2,)), DMA((2, 12)),
        ],
        compiler_params=pltpu.CompilerParams(collective_id=1, has_side_effects=True, vmem_limit_bytes=LIMIT),
        cost_estimate=WORK,
        name="finish_rows",
    )(part_a, res, bias, m_all, bias_g, bias_u, *pieces)


def solution(mesh):
    wd_count = mesh.shape['wd']
    ch_count = mesh.shape['ch']
    row_spec = P('dp', 'wd')
    specs = (row_spec, P('dp'), P('wd'), P('wd', 'ch'), P('ch'), P('wd', 'ch'), P('ch'), P(None, 'ch'), P('ch'), P('ch'), P('ch'), P('ch'), P('ch'), P('ch'), P('ch', 'wd'), P('wd'), P('wd'), P('wd', 'ch'), P('ch'), P('wd', 'ch'), P('ch'), P('ch', 'wd'), P('wd'))
    core_hop, y_hop, both_hop = (flip_pairs(wd_count, r) for r in OTHERS)

    def local_layer(resid_in, seg_pos, gain_temporal, w_x, bias_x, w_y, bias_y, conv_w, conv_bias, lam_param, rgate_w, rgate_b, igate_w, igate_b, w_o, bias_o, gain_mlp, w_g, bias_g, w_u, bias_u, w_d, bias_d):
        me, z, dp = lax.axis_index('wd'), lax.axis_index('ch'), lax.axis_index('dp')
        idx = jnp.stack([me, dp, z]).astype(jnp.int32)
        tokens, local_width = resid_in.shape
        model_width = local_width * wd_count
        chunk = tokens // CHUNKS
        share = tokens // (ch_count * wd_count)
        rows = share // SUB
        channels = w_x.shape[1] // wd_count

        def half_from_y(w):
            half = w.shape[0] // 2
            part = lax.dynamic_slice_in_dim(w, dp * half, half, 0)
            return lax.ppermute(part, 'wd', y_hop)

        def gathered(w):
            far_a = half_from_y(w)
            far_b = lax.ppermute(far_a, 'dp', flip_pairs(2, 1))
            core = lax.ppermute(w, 'wd', core_hop)
            both_a = lax.ppermute(far_a, 'wd', core_hop)
            both_b = lax.ppermute(far_b, 'wd', core_hop)
            return w, core, far_a, far_b, both_a, both_b

        vecs = jnp.stack([bias_o, gain_mlp, bias_d])
        vecs = [vecs] + [lax.ppermute(vecs, 'wd', hop) for hop in (core_hop, y_hop, both_hop)]
        vecs = jnp.stack(vecs).astype(F32)[:, :, None, :]
        bias_o_r, gain_r, bias_d_r = vecs[:, 0], vecs[:, 1], vecs[:, 2]

        blocks = resid_in.reshape(ch_count, wd_count, share, local_width)
        line = lax.dynamic_index_in_dim(blocks, z, 0, keepdims=False)
        x_rows = [lax.dynamic_index_in_dim(line, me ^ r, 0, keepdims=False) for r in range(4)]
        early = []
        for r, hop in zip(OTHERS, (core_hop, y_hop, both_hop)):
            early.append(lax.ppermute(x_rows[r], 'wd', hop))
        x_rows = [x_rows[0]] + early

        resid32 = resid_in.astype(F32)
        sum_sq = lax.psum(jnp.sum(resid32 * resid32, axis=1, keepdims=True), 'wd')
        normed = (resid32 * lax.rsqrt(sum_sq / model_width + EPS) * (1.0 + gain_temporal.astype(F32))).astype(BF16)

        cols = lambda arr, r: lax.dynamic_slice_in_dim(arr, (me ^ r) * channels, channels, arr.ndim - 1)
        wxy = [jnp.concatenate([cols(w_x, r), cols(w_y, r)], axis=1) for r in range(4)]
        w_send = jnp.concatenate([wxy[1], wxy[3]], axis=1)
        mine = lambda arr: cols(arr.astype(F32)[None], 0)
        bias_xy = jnp.concatenate([mine(bias_x), mine(bias_y)], axis=1)
        conv = jnp.concatenate([cols(conv_w.astype(F32), 0), mine(conv_bias), jnp.zeros((3, channels), F32)], axis=0)
        soft = jax.nn.softplus(-mine(lam_param))
        block = lambda arr: lax.dynamic_index_in_dim(arr, me, 0, keepdims=False)
        gate_w = jnp.concatenate([block(rgate_w), block(igate_w)], axis=1)
        gate_b = jnp.concatenate([mine(rgate_b), mine(igate_b)], axis=1)
        pos = seg_pos.reshape(tokens, 1)

        w_o_parts = gathered(w_o)

        tail = jnp.zeros((GROUP, channels), F32)
        carry = jnp.zeros((GROUP, channels), F32)
        for k in range(CHUNKS):
            n = lax.slice_in_dim(normed, k * chunk, (k + 1) * chunk, axis=0)
            sent = dot32(n, w_send).astype(BF16)
            sent = lax.ppermute(sent, 'wd', core_hop)
            far = (dot32(n, wxy[2]) + sent[:, 2 * channels:].astype(F32)).astype(BF16)
            far = lax.ppermute(far, 'wd', y_hop)
            own = dot32(n, wxy[0]).astype(BF16)
            mixed, tail, carry = lru(idx, own, sent, far, pos[k * chunk:(k + 1) * chunk], bias_xy, conv, soft, gate_w, gate_b, tail, carry, share)
            if k == 0:
                mix_in = [mixed[0]] + [lax.ppermute(mixed[r], 'wd', hop) for r, hop in zip(OTHERS, (core_hop, y_hop, both_hop))]
        x_rows = [x.reshape(SUB, rows, local_width) for x in x_rows]
        res, m, got = residual_norm(ch_count, x_rows, bias_o_r, gain_r, mixed, mix_in, w_o_parts, [w_g, w_u, w_d])
        g_parts, u_parts, d_parts = ([w, core, far_a, far_b, both_a, both_b] for w, (far_a, core, both_a, far_b, both_b) in zip((w_g, w_u, w_d), got))
        bias_gu = [b.astype(F32)[None] for b in (bias_g, bias_u)]
        inner = gate_up(idx, m, g_parts, u_parts, *bias_gu, TILE)
        d_part = partial_rows(down_body, idx, inner, d_parts, (ch_count, SUB // 2, rows), TILE)
        return finish_rows(ch_count, d_part, res, bias_d_r, m, *bias_gu, g_parts + u_parts + d_parts).reshape(tokens, local_width)

    return jax.shard_map(local_layer, mesh=mesh, in_specs=specs, out_specs=row_spec, check_vma=False)
```

```python
import functools

import jax
import jax.numpy as jnp
from jax import lax
from jax.experimental import pallas as pl
from jax.experimental.pallas import tpu as pltpu
from jax.sharding import PartitionSpec as P


EPS = 1e-6
SPLIT = (3, 1)
SUB = 16
TILE = 512
PIECES = 4
GROUP = 8
WAYS = (0, 1)
BLOCKS = (0, 1, 2, 3)
OTHERS = BLOCKS[1:]
LIMIT = 60 * 2 ** 20
WORK = pl.CostEstimate(flops=2 * 10 ** 11, bytes_accessed=2 * 10 ** 7, transcendentals=0)
MESH = pl.DeviceIdType.MESH
F32 = jnp.float32
BF16 = jnp.bfloat16


def flip_pairs(count, r):
    return [(i, i ^ r) for i in range(count)]


def dot32(a, b):
    return jnp.dot(a, b, preferred_element_type=F32)


def lru_body(idx_ref, own_ref, peer_ref, far_ref, pos_ref, bias_ref, conv_ref, sp_ref, gate_w_ref, gate_b_ref, tail_ref, carry_ref, mixed_ref, tail_out, carry_out, ubuf, abuf, bbuf, carry):
    step = pl.program_id(0)
    rows, width = abuf.shape

    @pl.when(step == 0)
    def _():
        ubuf[:GROUP, :] = tail_ref[...]
        carry[...] = carry_ref[...]

    @pl.when(step > 0)
    def _():
        ubuf[:GROUP, :] = ubuf[rows:, :]

    total = own_ref[...].astype(F32) + peer_ref[...].astype(F32) + far_ref[...].astype(F32) + bias_ref[...]
    ubuf[GROUP:, :] = total[:, :width].astype(BF16).astype(F32)
    pos = pos_ref[...]
    conv = conv_ref[4:5, :] + ubuf[GROUP:, :] * conv_ref[0:1, :]
    for shift in OTHERS:
        moved = ubuf[GROUP - shift:rows + GROUP - shift, :]
        conv = conv + jnp.where(pos >= shift, moved, 0.0) * conv_ref[shift:shift + 1, :]
    conv_b = conv.astype(BF16)
    conv32 = conv_b.astype(F32)
    gates = jax.nn.sigmoid(dot32(conv_b, gate_w_ref[...]) + gate_b_ref[...])
    rate = gates[:, :width]
    inflow = gates[:, width:]
    depth = 8.0 * rate * sp_ref[...]
    twice = 2.0 * depth
    series = 1.0
    for k in (5, 4, 3, 2):
        series = 1.0 - (twice * series) / k
    series = twice * series
    left = jnp.where(twice < 0.125, series, 1.0 - jnp.exp(-twice))
    reset = pos == 0
    abuf[...] = jnp.where(reset, 0.0, jnp.exp(-depth))
    bbuf[...] = jnp.where(reset, 1.0, jnp.sqrt(left)) * inflow * conv32

    row = lax.broadcasted_iota(jnp.int32, (GROUP, width), 0)

    def group(g, held):
        at = pl.multiple_of(g * GROUP, GROUP)
        a = abuf[pl.ds(at, GROUP), :]
        b = bbuf[pl.ds(at, GROUP), :]
        for d in (1, 2, 4):
            keep = row >= d
            b = b + a * jnp.where(keep, pltpu.roll(b, d, 0), 0.0)
            a = a * jnp.where(keep, pltpu.roll(a, d, 0), 1.0)
        bbuf[pl.ds(at, GROUP), :] = b + a * held
        last_a = jnp.broadcast_to(a[GROUP - 1:, :], (GROUP, width))
        last_b = jnp.broadcast_to(b[GROUP - 1:, :], (GROUP, width))
        return last_b + last_a * held

    held = lax.fori_loop(0, rows // GROUP, group, carry[...], unroll=GROUP)
    carry[...] = held
    y_branch = jax.nn.gelu(total[:, width:], approximate=True).astype(BF16)
    mixed_ref[...] = (bbuf[...] * y_branch.astype(F32)).astype(BF16).reshape(mixed_ref.shape)
    tail_out[...] = ubuf[rows:, :]
    carry_out[...] = held


def lru(idx, own, peer, far, pos, bias, conv, sp, gate_w, gate_b, tail, carry, rows):
    tokens = own.shape[0]
    width = own.shape[1] // 2
    blocks = tokens // rows
    wide = pl.BlockSpec((rows, 2 * width), lambda s, idx: (s, 0))
    full = lambda arr: pl.BlockSpec(arr.shape, lambda s, idx: (0,) * arr.ndim)
    state = jax.ShapeDtypeStruct((GROUP, width), F32)
    return pl.pallas_call(
        lru_body,
        grid_spec=pltpu.PrefetchScalarGridSpec(
            num_scalar_prefetch=1,
            grid=(blocks,),
            in_specs=[wide, wide, wide, pl.BlockSpec((rows, 1), lambda s, idx: (s, 0))] + [full(v) for v in (bias, conv, sp, gate_w, gate_b, tail, carry)],
            out_specs=[pl.BlockSpec((1, 1, rows, width), lambda s, idx: ((s % 4) ^ idx[0], s // 4, 0, 0)), full(tail), full(carry)],
            scratch_shapes=[pltpu.VMEM((rows + GROUP, width), F32), pltpu.VMEM((rows, width), F32), pltpu.VMEM((rows, width), F32), pltpu.VMEM((GROUP, width), F32)],
        ),
        out_shape=[jax.ShapeDtypeStruct((4, blocks // 4, rows, width), BF16), state, state],
        compiler_params=pltpu.CompilerParams(dimension_semantics=("arbitrary",)),
        cost_estimate=pl.CostEstimate(flops=tokens * width * 4000, bytes_accessed=tokens * width * 20, transcendentals=tokens * width * 8),
        name="lru",
    )(idx, own, peer, far, pos, bias, conv, sp, gate_w, gate_b, tail, carry)


def line_body(kind, n_ship, *refs):
    if kind == "norm":
        x_rows, (bias, gain, mixed), mix_in, o_parts = refs[:4], refs[4:7], refs[7:11], refs[11:17]
        ship, refs = refs[17:17 + n_ship], refs[17 + n_ship:]
        res_ref, out = refs[:2]
        shipped, refs = refs[2:2 + 5 * n_ship], refs[2 + 5 * n_ship:]
        rbuf, obuf, send, recv, loc, w_send, w_recv, part, mixbuf, wo, a_send, a_recv, pre_sem = refs
    else:
        res_ref, bias, m_all, bias_g, bias_u = refs[:5]
        g_parts, u_parts, d_parts = refs[5:11], refs[11:17], refs[17:23]
        out, late_b, late_both, rbuf, obuf, send, recv, loc, a_send, a_recv, part, mbuf, inner, wbuf, pre_sem, tile_sem, l_send, l_recv = refs[23:]
    n = rbuf.shape[1] + 1
    steps = rbuf.shape[2]
    z, me, dp = lax.axis_index('ch'), lax.axis_index('wd'), lax.axis_index('dp')
    lag = 0 if kind == "norm" else 1
    wd_to = lambda r: {'wd': me ^ r}
    peers = [wd_to(r) for r in OTHERS] + [{'dp': 1 - dp}]

    barrier = pltpu.get_barrier_semaphore()
    for peer in peers:
        pl.semaphore_signal(barrier, inc=1, device_id=peer, device_id_type=MESH)

    @pl.when(z > 0)
    def _():
        pl.semaphore_signal(barrier, inc=1, device_id={'ch': z - 1}, device_id_type=MESH)

    @pl.when(z < n - 1)
    def _():
        pl.semaphore_signal(barrier, inc=1, device_id={'ch': z + 1}, device_id_type=MESH)

    @pl.when((z > 0) & (z < n - 1))
    def _():
        pl.semaphore_wait(barrier, len(peers) + 2)

    @pl.when((z == 0) | (z == n - 1))
    def _():
        pl.semaphore_wait(barrier, len(peers) + 1)

    place = lambda way: z if way == 0 else n - 1 - z
    there = lambda way, p: p if way == 0 else n - 1 - p

    def hop(way, slot, s, src, dst):
        return pltpu.make_async_remote_copy(src_ref=src, dst_ref=dst, send_sem=send.at[way, slot, s], recv_sem=recv.at[way, slot, s], device_id={'ch': there(way, jnp.minimum(place(way) + 1, n - 1))}, device_id_type=MESH)

    def reduce_hop(way, h, s, first):
        src = part.at[there(way, place(way) + n - h), s] if first else rbuf.at[way, h - 2, s]
        return hop(way, h - 1, s, src, rbuf.at[way, h - 1, s])

    def reduce_wait(way, h, s):
        at = rbuf.at[way, h - 1, s]
        hop(way, h - 1, s, at, at).wait_recv()

    def block_at(o, s):
        return out.at[o, s] if kind == "norm" else out.at[o, :, s]

    def gather_hop(way, h, s):
        at = block_at(there(way, place(way) - (h - 1)), s)
        src = obuf.at[s] if kind == "norm" and h == 1 else at
        return hop(way, n - 2 + h, s, src, at)

    def local_copy(s):
        src, dst = (obuf.at[s], out.at[z, s]) if kind == "norm" else (obuf.at[s, me], out.at[z, me, s])
        return pltpu.make_async_copy(src, dst, loc.at[s])

    def swap(r, s):
        return pltpu.make_async_remote_copy(src_ref=obuf.at[s, me ^ r], dst_ref=out.at[z, me, s], send_sem=a_send.at[r - 1, s], recv_sem=a_recv.at[r - 1, s], device_id=wd_to(r), device_id_type=MESH)

    def swapped(r, s):
        return pltpu.make_async_remote_copy(src_ref=obuf.at[s, me ^ r], dst_ref=out.at[z, me ^ r, s], send_sem=a_send.at[r - 1, s], recv_sem=a_recv.at[r - 1, s], device_id=wd_to(r), device_id_type=MESH)

    def weight_copy(q, j):
        i, p = q // PIECES, q % PIECES
        far_a, core, both_a, far_b, both_b = shipped[5 * i:5 * i + 5]
        size = far_a.shape[0] // PIECES
        own_at, at = pl.ds((PIECES * dp + p) * size, size), pl.ds(p * size, size)
        if j == 4:
            src, dst = ship[i], core
        elif j == 0:
            src, dst = ship[i].at[own_at], far_a.at[at]
        else:
            src, dst = ((far_a, far_b), (far_a, both_a), (far_b, both_b))[j - 1]
            src, dst = src.at[at], dst.at[at]
        to = (wd_to(2), {'dp': 1 - dp}, wd_to(1), wd_to(1), wd_to(1))[j]
        return pltpu.make_async_remote_copy(src_ref=src, dst_ref=dst, send_sem=w_send.at[q, j], recv_sem=w_recv.at[q, j], device_id=to, device_id_type=MESH)

    def row_places(pieces):
        own, core, far_a, far_b, both_a, both_b = pieces
        size, part_size = own.shape[0], far_a.shape[0]
        return ((own, 0), (core, size), (far_a, 2 * size + dp * part_size), (far_b, 2 * size + (1 - dp) * part_size), (both_a, 3 * size + dp * part_size), (both_b, 3 * size + (1 - dp) * part_size))

    def mix_copy(r, landed):
        there_at = mixbuf.at[me ^ r if landed else me, pl.ds(n - mixed.shape[1], mixed.shape[1])]
        return pltpu.make_async_remote_copy(src_ref=mixed.at[r], dst_ref=there_at, send_sem=a_send.at[r - 1], recv_sem=a_recv.at[r - 1], device_id=wd_to(r), device_id_type=MESH)

    if kind == "norm":
        for r in OTHERS:
            mix_copy(r, False).start()
        jobs = [(mixed.at[0], mixbuf.at[me, pl.ds(n - mixed.shape[1], mixed.shape[1])])]
        jobs += [(src, mixbuf.at[me ^ r, pl.ds(0, src.shape[0])]) for r, src in enumerate(mix_in)]
        jobs += [(w, wo.at[pl.ds(to, w.shape[0])]) for w, to in row_places(o_parts)]
        loads = [pltpu.make_async_copy(src, dst, pre_sem.at[j]) for j, (src, dst) in enumerate(jobs)]
        for copy in loads:
            copy.start()
        for q in range(PIECES * n_ship):
            weight_copy(q, 0).start()
        for i in range(n_ship):
            weight_copy(PIECES * i, 4).start()

        def project(j, _):
            d, r = lax.div(j, 4), lax.rem(j, 4)
            depth = mixbuf.shape[3]
            acc = None
            for b in BLOCKS:
                at = pl.ds(pl.multiple_of((4 * r + b) * depth, depth), depth)
                val = dot32(mixbuf[b, d], wo[at, :])
                acc = val if acc is None else acc + val
            part[d, :, r] = acc.astype(BF16).reshape(steps, part.shape[3], part.shape[4])
            return 0

        for copy in loads:
            copy.wait()
        first = 4 * mix_in[0].shape[0]
        lax.fori_loop(0, first, project, 0)
        for r in OTHERS:
            mix_copy(r, True).wait_recv()
        lax.fori_loop(first, 4 * n, project, 0)

    crossed = PIECES * n_ship - PIECES // 2
    half = steps // 2
    if kind != "norm":
        gates = inner.shape[1] // TILE
        per_block = part.shape[4] // TILE
        tiles = gates + 4 * per_block
        loads = [pltpu.make_async_copy(m_all.at[:, pl.ds(i * half, half)], mbuf.at[i], pre_sem.at[i]) for i in WAYS]

        def tile_copies(q, down_block):
            slot = lax.rem(q, 2)
            if down_block is None:
                at = pl.ds(pl.multiple_of(q * TILE, TILE), TILE)
                jobs = [(w, i, to) for i, pieces in enumerate((g_parts, u_parts)) for w, to in row_places(pieces)]
            else:
                at = pl.ds(pl.multiple_of(lax.rem(q - gates, per_block) * TILE, TILE), TILE)
                own, core, far_a, far_b, both_a, both_b = d_parts
                rows_a = dp * far_a.shape[0]
                rows_b = far_a.shape[0] - rows_a
                late = rows_b + far_b.shape[0]
                jobs = ([(own, 0, 0)], [(core, 0, 0)], [(far_a, 0, rows_a), (far_b, 0, rows_b), (late_b, 0, late)], [(both_a, 0, rows_a), (both_b, 0, rows_b), (late_both, 0, late)])[down_block]
            return [pltpu.make_async_copy(w.at[:, at], wbuf.at[slot, i, pl.ds(to, w.shape[0]), :], tile_sem.at[slot, j]) for j, (w, i, to) in enumerate(jobs)]

        def for_tile(q, act):
            @pl.when(q < gates)
            def _():
                for copy in tile_copies(q, None):
                    act(copy)

            for r in BLOCKS:
                @pl.when((q >= gates + r * per_block) & (q < gates + (r + 1) * per_block))
                def _(r=r):
                    for copy in tile_copies(q, r):
                        act(copy)

        def late_copy(j):
            far_a, size = d_parts[2], late_b.shape[0]
            src, dst, to = ((far_a.at[pl.ds(size, size)], late_b, {'dp': 1 - dp}), (late_b, late_both, wd_to(1)))[j]
            return pltpu.make_async_remote_copy(src_ref=src, dst_ref=dst, send_sem=l_send.at[j], recv_sem=l_recv.at[j], device_id=to, device_id_type=MESH)

        late_copy(0).start()

        def mlp_tile(job, _):
            phase, q = lax.div(job, tiles), lax.rem(job, tiles)

            @pl.when(job == gates + per_block)
            def _():
                late_copy(0).wait_recv()
                late_copy(1).start()

            @pl.when(job == gates + 3 * per_block - 1)
            def _():
                late_copy(1).wait_recv()

            for_tile(q, lambda copy: copy.wait())

            @pl.when(job < 2 * tiles - 1)
            def _():
                for_tile(lax.rem(job + 1, tiles), lambda copy: copy.start())

            slot = lax.rem(q, 2)
            toks = inner.shape[0]

            @pl.when(q < gates)
            def _():
                at = pl.ds(pl.multiple_of(q * TILE, TILE), TILE)
                sums = []
                for i in range(2):
                    sums.append(dot32(mbuf[phase].reshape(toks, mbuf.shape[4]), wbuf[slot, i]))
                gate = jax.nn.gelu(sums[0] + bias_g[:, at], approximate=True)
                inner[:, at] = (gate * (sums[1] + bias_u[:, at])).astype(BF16)

            @pl.when(q >= gates)
            def _():
                d = q - gates
                at = pl.ds(pl.multiple_of(lax.rem(d, per_block) * TILE, TILE), TILE)
                val = dot32(inner[...], wbuf[slot, 0, 0:inner.shape[1], :]).astype(BF16)
                part[:, pl.ds(phase * half, half), lax.div(d, per_block), :, at] = val.reshape(n, half, part.shape[3], TILE)

            return 0

        for copy in loads:
            copy.start()
        for_tile(0 * z, lambda copy: copy.start())
        loads[0].wait()
        lax.fori_loop(0, tiles, mlp_tile, 0)
        loads[1].wait()

    def finish(s):
        for way in WAYS:
            p = place(way)

            @pl.when(p > 0)
            def _(way=way):
                reduce_wait(way, n - 1, s)

        total = 0.0
        for r in BLOCKS:
            val = part[z, s, r].astype(F32)
            val = val + jnp.where(z > 0, rbuf[0, n - 2, s, r].astype(F32), 0.0)
            val = val + jnp.where(z < n - 1, rbuf[1, n - 2, s, r].astype(F32), 0.0)
            if kind == "norm":
                val = x_rows[r][s].astype(F32) + val + bias[r]
                res_ref[s, r] = val
                total = total + jnp.sum(val * val, axis=1, keepdims=True)
            else:
                obuf[s, me ^ r] = (res_ref[s, r] + val + bias[r]).astype(BF16)
        if kind == "norm":
            width = res_ref.shape[3]
            scale = lax.rsqrt(total / (4 * width) + EPS)
            for r in BLOCKS:
                normed = (res_ref[s, r] * scale * (1.0 + gain[r])).astype(BF16)
                obuf[s, :, r * width:(r + 1) * width] = normed
        else:
            for r in OTHERS:
                swap(r, s).start()
        local_copy(s).start()

    def step(t, _):
        for h in range(n, 0, -1):
            s = t - (n - 1) - lag - (h - 1)

            @pl.when((s >= 0) & (s < steps))
            def _(h=h, s=s):
                if h == 1 and kind != "norm":
                    for r in OTHERS:
                        swapped(r, s).wait_recv()
                    local_copy(s).wait()
                if h == 1 and kind == "norm":
                    finish(s)
                for way in WAYS:
                    p = place(way)
                    if h > 1:
                        @pl.when(p >= h - 1)
                        def _(way=way):
                            at = block_at(there(way, place(way) - (h - 1)), s)
                            hop(way, n - 3 + h, s, at, at).wait_recv()
                    if h < n:
                        @pl.when((p >= h - 1) & (p < n - 1))
                        def _(way=way):
                            gather_hop(way, h, s).start()

        if lag:
            s = t - (n - 1)

            @pl.when((s >= 0) & (s < steps))
            def _(s=s):
                finish(s)

        for h in range(n - 1, 0, -1):
            s = t - (h - 1)
            for way in WAYS:
                p = place(way)

                @pl.when((s >= 0) & (s < steps) & (p < h))
                def _(h=h, s=s, way=way, p=p):
                    if h > 1:
                        @pl.when(p > 0)
                        def _():
                            reduce_wait(way, h - 1, s)
                            mine = part[there(way, p + n - h), s].astype(F32)
                            rbuf[way, h - 2, s] = (rbuf[way, h - 2, s].astype(F32) + mine).astype(BF16)
                            reduce_hop(way, h, s, False).start()

                    @pl.when(p == 0)
                    def _():
                        reduce_hop(way, h, s, True).start()

        if kind != "norm":
            @pl.when(t < half)
            def _():
                lax.fori_loop(tiles + lax.div(t * tiles, half), tiles + lax.div((t + 1) * tiles, half), mlp_tile, 0)

        if kind == "norm":
            for q in range(PIECES * n_ship):
                @pl.when(t == (3 * q + 5) // 2)
                def _(q=q):
                    weight_copy(q, 0).wait_recv()
                    if q < crossed:
                        weight_copy(q, 1).start()
                    weight_copy(q, 2).start()

                if q < crossed:
                    @pl.when(t == (3 * q + 10) // 2)
                    def _(q=q):
                        weight_copy(q, 1).wait_recv()
                        weight_copy(q, 3).start()
        return 0

    lax.fori_loop(0, steps + 2 * n - 2 + lag, step, 0)

    def drain(s, _):
        for way in WAYS:
            p = place(way)
            for h in range(1, n):
                @pl.when(p < h)
                def _(way=way, h=h):
                    reduce_hop(way, h, s, True).wait_send()

                @pl.when((p >= h - 1) & (p < n - 1))
                def _(way=way, h=h):
                    gather_hop(way, h, s).wait_send()
        if kind == "norm":
            local_copy(s).wait()
        else:
            for r in OTHERS:
                swap(r, s).wait_send()
        return 0

    if kind != "norm":
        for j in WAYS:
            late_copy(j).wait_send()

    lax.fori_loop(0, steps, drain, 0)
    if kind == "norm":
        for q in range(PIECES * n_ship):
            weight_copy(q, 0).wait_send()
            weight_copy(q, 2).wait()
            if q < crossed:
                weight_copy(q, 1).wait_send()
                weight_copy(q, 3).wait()
        for i in range(n_ship):
            weight_copy(PIECES * i, 4).wait()
        for r in OTHERS:
            mix_copy(r, False).wait_send()


VM = pl.BlockSpec(memory_space=pltpu.VMEM)
ANY = pl.BlockSpec(memory_space=pl.ANY)
DMA = pltpu.SemaphoreType.DMA


def line_scratch(n, steps, block, done):
    sems = (2, 2 * n - 2, steps)
    return [pltpu.VMEM((2, n - 1, steps) + block, BF16), pltpu.VMEM((steps,) + done, BF16), DMA(sems), DMA(sems), DMA((steps,))]


def residual_norm(n, xs, bias, gain, mixed, mix_in, o_parts, ship):
    steps, rows, width = xs[0].shape
    out_w = []
    for w in ship:
        half = jax.ShapeDtypeStruct((w.shape[0] // 2, w.shape[1]), BF16)
        if w is ship[-1]:
            late = jax.ShapeDtypeStruct((w.shape[0] // 4, w.shape[1]), BF16)
        else:
            late = half
        out_w += [half, jax.ShapeDtypeStruct(w.shape, BF16), half, late, late]
    done = (rows, 4 * width)
    far = [mixed, *mix_in, *o_parts, *ship]
    pieces = PIECES * len(ship)
    outs = pl.pallas_call(
        functools.partial(line_body, "norm", len(ship)),
        in_specs=[VM] * 6 + [ANY] * len(far),
        out_specs=[VM, ANY] + [ANY] * len(out_w),
        out_shape=[jax.ShapeDtypeStruct((steps, 4, rows, width), F32), jax.ShapeDtypeStruct((n, steps) + done, BF16)] + out_w,
        scratch_shapes=line_scratch(n, steps, (4, rows, width), done) + [
            DMA((pieces, 5)), DMA((pieces, 5)),
            pltpu.VMEM((n, steps, 4, rows, width), BF16),
            pltpu.VMEM((4, n) + mixed.shape[2:], BF16),
            pltpu.VMEM((4 * width, width), BF16),
            DMA((3,)), DMA((3,)), DMA((11,)),
        ],
        compiler_params=pltpu.CompilerParams(collective_id=0, has_side_effects=True, vmem_limit_bytes=LIMIT),
        cost_estimate=WORK,
        name="residual_norm",
    )(*xs, bias, gain, *far)
    return outs[0], outs[1], [outs[2 + 5 * i:7 + 5 * i] for i in range(len(ship))]


def finish_rows(n, res, bias, m_all, bias_g, bias_u, pieces):
    steps, _, rows, width = res.shape
    half = steps // 2
    inner_width = bias_g.shape[1]
    toks = n * half * rows
    return pl.pallas_call(
        functools.partial(line_body, "finish", 0),
        in_specs=[VM, VM, ANY, VM, VM] + [ANY] * len(pieces),
        out_specs=[ANY] * 3,
        out_shape=[jax.ShapeDtypeStruct((n, 4, steps, rows, width), BF16)] + [jax.ShapeDtypeStruct(pieces[-1].shape, BF16)] * 2,
        scratch_shapes=line_scratch(n, steps, (4, rows, width), (4, rows, width)) + [
            DMA((3, steps)), DMA((3, steps)),
            pltpu.VMEM((n, steps, 4, rows, width), BF16),
            pltpu.VMEM((2, n, half) + m_all.shape[2:], BF16),
            pltpu.VMEM((toks, inner_width), BF16),
            pltpu.VMEM((2, 2, 4 * width, TILE), BF16),
            DMA((2,)), DMA((2, 12)), DMA((2,)), DMA((2,)),
        ],
        compiler_params=pltpu.CompilerParams(collective_id=1, has_side_effects=True, vmem_limit_bytes=LIMIT),
        cost_estimate=WORK,
        name="finish_rows",
    )(res, bias, m_all, bias_g, bias_u, *pieces)[0]


def solution(mesh):
    wd_count = mesh.shape['wd']
    ch_count = mesh.shape['ch']
    row_spec = P('dp', 'wd')
    specs = (row_spec, P('dp'), P('wd'), P('wd', 'ch'), P('ch'), P('wd', 'ch'), P('ch'), P(None, 'ch'), P('ch'), P('ch'), P('ch'), P('ch'), P('ch'), P('ch'), P('ch', 'wd'), P('wd'), P('wd'), P('wd', 'ch'), P('ch'), P('wd', 'ch'), P('ch'), P('ch', 'wd'), P('wd'))
    core_hop, y_hop, both_hop = (flip_pairs(wd_count, r) for r in OTHERS)

    def local_layer(resid_in, seg_pos, gain_temporal, w_x, bias_x, w_y, bias_y, conv_w, conv_bias, lam_param, rgate_w, rgate_b, igate_w, igate_b, w_o, bias_o, gain_mlp, w_g, bias_g, w_u, bias_u, w_d, bias_d):
        me, z, dp = lax.axis_index('wd'), lax.axis_index('ch'), lax.axis_index('dp')
        idx = jnp.stack([me, dp, z]).astype(jnp.int32)
        tokens, local_width = resid_in.shape
        model_width = local_width * wd_count
        unit = tokens // sum(SPLIT)
        share = tokens // (ch_count * wd_count)
        rows = share // SUB
        channels = w_x.shape[1] // wd_count

        def half_from_y(w):
            half = w.shape[0] // 2
            part = lax.dynamic_slice_in_dim(w, dp * half, half, 0)
            return lax.ppermute(part, 'wd', y_hop)

        def gathered(w):
            far_a = half_from_y(w)
            far_b = lax.ppermute(far_a, 'dp', flip_pairs(2, 1))
            core = lax.ppermute(w, 'wd', core_hop)
            both_a = lax.ppermute(far_a, 'wd', core_hop)
            both_b = lax.ppermute(far_b, 'wd', core_hop)
            return w, core, far_a, far_b, both_a, both_b

        vecs = jnp.stack([bias_o, gain_mlp, bias_d])
        vecs = [vecs] + [lax.ppermute(vecs, 'wd', hop) for hop in (core_hop, y_hop, both_hop)]
        vecs = jnp.stack(vecs).astype(F32)[:, :, None, :]
        bias_o_r, gain_r, bias_d_r = vecs[:, 0], vecs[:, 1], vecs[:, 2]

        blocks = resid_in.reshape(ch_count, wd_count, share, local_width)
        line = lax.dynamic_index_in_dim(blocks, z, 0, keepdims=False)
        x_rows = [lax.dynamic_index_in_dim(line, me ^ r, 0, keepdims=False) for r in range(4)]
        early = []
        for r, hop in zip(OTHERS, (core_hop, y_hop, both_hop)):
            early.append(lax.ppermute(x_rows[r], 'wd', hop))
        x_rows = [x_rows[0]] + early

        resid32 = resid_in.astype(F32)
        sum_sq = lax.psum(jnp.sum(resid32 * resid32, axis=1, keepdims=True), 'wd')
        normed = (resid32 * lax.rsqrt(sum_sq / model_width + EPS) * (1.0 + gain_temporal.astype(F32))).astype(BF16)

        cols = lambda arr, r: lax.dynamic_slice_in_dim(arr, (me ^ r) * channels, channels, arr.ndim - 1)
        wxy = [jnp.concatenate([cols(w_x, r), cols(w_y, r)], axis=1) for r in range(4)]
        w_send = jnp.concatenate([wxy[1], wxy[3]], axis=1)
        mine = lambda arr: cols(arr.astype(F32)[None], 0)
        bias_xy = jnp.concatenate([mine(bias_x), mine(bias_y)], axis=1)
        conv = jnp.concatenate([cols(conv_w.astype(F32), 0), mine(conv_bias), jnp.zeros((3, channels), F32)], axis=0)
        soft = jax.nn.softplus(-mine(lam_param))
        block = lambda arr: lax.dynamic_index_in_dim(arr, me, 0, keepdims=False)
        gate_w = jnp.concatenate([block(rgate_w), block(igate_w)], axis=1)
        gate_b = jnp.concatenate([mine(rgate_b), mine(igate_b)], axis=1)
        pos = seg_pos.reshape(tokens, 1)

        w_o_parts = gathered(w_o)

        tail = jnp.zeros((GROUP, channels), F32)
        carry = jnp.zeros((GROUP, channels), F32)
        for k, size in enumerate(SPLIT):
            start, stop = sum(SPLIT[:k]) * unit, sum(SPLIT[:k + 1]) * unit
            n = lax.slice_in_dim(normed, start, stop, axis=0)
            sent = dot32(n, w_send).astype(BF16)
            sent = lax.ppermute(sent, 'wd', core_hop)
            far = (dot32(n, wxy[2]) + sent[:, 2 * channels:].astype(F32)).astype(BF16)
            far = lax.ppermute(far, 'wd', y_hop)
            own = dot32(n, wxy[0]).astype(BF16)
            mixed, tail, carry = lru(idx, own, sent, far, pos[start:stop], bias_xy, conv, soft, gate_w, gate_b, tail, carry, share)
            if k == 0:
                mix_in = [mixed[0]] + [lax.ppermute(mixed[r], 'wd', hop) for r, hop in zip(OTHERS, (core_hop, y_hop, both_hop))]
        x_rows = [x.reshape(SUB, rows, local_width) for x in x_rows]
        res, m, got = residual_norm(ch_count, x_rows, bias_o_r, gain_r, mixed, mix_in, w_o_parts, [w_g, w_u, w_d])
        g_parts, u_parts, d_parts = ([w, core, far_a, far_b, both_a, both_b] for w, (far_a, core, both_a, far_b, both_b) in zip((w_g, w_u, w_d), got))
        bias_gu = [b.astype(F32)[None] for b in (bias_g, bias_u)]
        return finish_rows(ch_count, res, bias_d_r, m, *bias_gu, g_parts + u_parts + d_parts).reshape(tokens, local_width)

    return jax.shard_map(local_layer, mesh=mesh, in_specs=specs, out_specs=row_spec, check_vma=False)
```

```python
import functools

import jax
import jax.numpy as jnp
from jax import lax
from jax.experimental import pallas as pl
from jax.experimental.pallas import tpu as pltpu
from jax.sharding import PartitionSpec as P


EPS = 1e-6
SPLIT = (3, 1)
SUB = 16
TILE = 512
PIECES = 4
GROUP = 8
WAYS = (0, 1)
BLOCKS = (0, 1, 2, 3)
OTHERS = BLOCKS[1:]
LIMIT = 60 * 2 ** 20
WORK = pl.CostEstimate(flops=2 * 10 ** 11, bytes_accessed=2 * 10 ** 7, transcendentals=0)
MESH = pl.DeviceIdType.MESH
F32 = jnp.float32
BF16 = jnp.bfloat16


def flip_pairs(count, r):
    return [(i, i ^ r) for i in range(count)]


def dot32(a, b):
    return jnp.dot(a, b, preferred_element_type=F32)


def lru_body(idx_ref, own_ref, peer_ref, far_ref, pos_ref, bias_ref, conv_ref, sp_ref, gate_w_ref, gate_b_ref, tail_ref, carry_ref, mixed_ref, tail_out, carry_out, ubuf, abuf, bbuf, carry):
    step = pl.program_id(0)
    rows, width = abuf.shape

    @pl.when(step == 0)
    def _():
        ubuf[:GROUP, :] = tail_ref[...]
        carry[...] = carry_ref[...]

    @pl.when(step > 0)
    def _():
        ubuf[:GROUP, :] = ubuf[rows:, :]

    total = own_ref[...].astype(F32) + peer_ref[...].astype(F32) + far_ref[...].astype(F32) + bias_ref[...]
    ubuf[GROUP:, :] = total[:, :width].astype(BF16).astype(F32)
    pos = pos_ref[...]
    conv = conv_ref[4:5, :] + ubuf[GROUP:, :] * conv_ref[0:1, :]
    for shift in OTHERS:
        moved = ubuf[GROUP - shift:rows + GROUP - shift, :]
        conv = conv + jnp.where(pos >= shift, moved, 0.0) * conv_ref[shift:shift + 1, :]
    conv_b = conv.astype(BF16)
    conv32 = conv_b.astype(F32)
    gates = jax.nn.sigmoid(dot32(conv_b, gate_w_ref[...]) + gate_b_ref[...])
    rate = gates[:, :width]
    inflow = gates[:, width:]
    depth = 8.0 * rate * sp_ref[...]
    twice = 2.0 * depth
    series = 1.0
    for k in (5, 4, 3, 2):
        series = 1.0 - (twice * series) / k
    series = twice * series
    left = jnp.where(twice < 0.125, series, 1.0 - jnp.exp(-twice))
    reset = pos == 0
    abuf[...] = jnp.where(reset, 0.0, jnp.exp(-depth))
    bbuf[...] = jnp.where(reset, 1.0, jnp.sqrt(left)) * inflow * conv32

    row = lax.broadcasted_iota(jnp.int32, (GROUP, width), 0)

    def group(g, held):
        at = pl.multiple_of(g * GROUP, GROUP)
        a = abuf[pl.ds(at, GROUP), :]
        b = bbuf[pl.ds(at, GROUP), :]
        for d in (1, 2, 4):
            keep = row >= d
            b = b + a * jnp.where(keep, pltpu.roll(b, d, 0), 0.0)
            a = a * jnp.where(keep, pltpu.roll(a, d, 0), 1.0)
        bbuf[pl.ds(at, GROUP), :] = b + a * held
        last_a = jnp.broadcast_to(a[GROUP - 1:, :], (GROUP, width))
        last_b = jnp.broadcast_to(b[GROUP - 1:, :], (GROUP, width))
        return last_b + last_a * held

    held = lax.fori_loop(0, rows // GROUP, group, carry[...], unroll=GROUP)
    carry[...] = held
    y_branch = jax.nn.gelu(total[:, width:], approximate=True).astype(BF16)
    mixed_ref[...] = (bbuf[...] * y_branch.astype(F32)).astype(BF16).reshape(mixed_ref.shape)
    tail_out[...] = ubuf[rows:, :]
    carry_out[...] = held


def lru(idx, own, peer, far, pos, bias, conv, sp, gate_w, gate_b, tail, carry, rows):
    tokens = own.shape[0]
    width = own.shape[1] // 2
    blocks = tokens // rows
    wide = pl.BlockSpec((rows, 2 * width), lambda s, idx: (s, 0))
    full = lambda arr: pl.BlockSpec(arr.shape, lambda s, idx: (0,) * arr.ndim)
    state = jax.ShapeDtypeStruct((GROUP, width), F32)
    return pl.pallas_call(
        lru_body,
        grid_spec=pltpu.PrefetchScalarGridSpec(
            num_scalar_prefetch=1,
            grid=(blocks,),
            in_specs=[wide, wide, wide, pl.BlockSpec((rows, 1), lambda s, idx: (s, 0))] + [full(v) for v in (bias, conv, sp, gate_w, gate_b, tail, carry)],
            out_specs=[pl.BlockSpec((1, 1, rows, width), lambda s, idx: ((s % 4) ^ idx[0], s // 4, 0, 0)), full(tail), full(carry)],
            scratch_shapes=[pltpu.VMEM((rows + GROUP, width), F32), pltpu.VMEM((rows, width), F32), pltpu.VMEM((rows, width), F32), pltpu.VMEM((GROUP, width), F32)],
        ),
        out_shape=[jax.ShapeDtypeStruct((4, blocks // 4, rows, width), BF16), state, state],
        compiler_params=pltpu.CompilerParams(dimension_semantics=("arbitrary",)),
        cost_estimate=pl.CostEstimate(flops=tokens * width * 4000, bytes_accessed=tokens * width * 20, transcendentals=tokens * width * 8),
        name="lru",
    )(idx, own, peer, far, pos, bias, conv, sp, gate_w, gate_b, tail, carry)


def line_body(kind, n_ship, *refs):
    if kind == "norm":
        (bias, gain, x_line, mixed), mix_in, o_parts = refs[:4], refs[4:8], refs[8:14]
        ship, refs = refs[14:14 + n_ship], refs[14 + n_ship:]
        res_ref, out = refs[:2]
        shipped, refs = refs[2:2 + 5 * n_ship], refs[2 + 5 * n_ship:]
        rbuf, obuf, send, recv, loc, w_send, w_recv, part, mixbuf, wo, a_send, a_recv, pre_sem, xbuf, x_send, x_recv = refs
    else:
        res_ref, bias, m_all, bias_g, bias_u = refs[:5]
        g_parts, u_parts, d_parts = refs[5:11], refs[11:17], refs[17:23]
        out, late_b, late_both, late_a, late_both_a, rbuf, obuf, send, recv, loc, a_send, a_recv, part, mbuf, inner, wbuf, pre_sem, tile_sem, l_send, l_recv = refs[23:]
    n = rbuf.shape[1] + 1
    steps = rbuf.shape[2]
    z, me, dp = lax.axis_index('ch'), lax.axis_index('wd'), lax.axis_index('dp')
    lag = 0 if kind == "norm" else 1
    wd_to = lambda r: {'wd': me ^ r}
    peers = [wd_to(r) for r in OTHERS] + [{'dp': 1 - dp}]

    barrier = pltpu.get_barrier_semaphore()
    for peer in peers:
        pl.semaphore_signal(barrier, inc=1, device_id=peer, device_id_type=MESH)

    @pl.when(z > 0)
    def _():
        pl.semaphore_signal(barrier, inc=1, device_id={'ch': z - 1}, device_id_type=MESH)

    @pl.when(z < n - 1)
    def _():
        pl.semaphore_signal(barrier, inc=1, device_id={'ch': z + 1}, device_id_type=MESH)

    @pl.when((z > 0) & (z < n - 1))
    def _():
        pl.semaphore_wait(barrier, len(peers) + 2)

    @pl.when((z == 0) | (z == n - 1))
    def _():
        pl.semaphore_wait(barrier, len(peers) + 1)

    place = lambda way: z if way == 0 else n - 1 - z
    there = lambda way, p: p if way == 0 else n - 1 - p

    def hop(way, slot, s, src, dst):
        return pltpu.make_async_remote_copy(src_ref=src, dst_ref=dst, send_sem=send.at[way, slot, s], recv_sem=recv.at[way, slot, s], device_id={'ch': there(way, jnp.minimum(place(way) + 1, n - 1))}, device_id_type=MESH)

    def reduce_hop(way, h, s, first):
        src = part.at[there(way, place(way) + n - h), s] if first else rbuf.at[way, h - 2, s]
        return hop(way, h - 1, s, src, rbuf.at[way, h - 1, s])

    def reduce_wait(way, h, s):
        at = rbuf.at[way, h - 1, s]
        hop(way, h - 1, s, at, at).wait_recv()

    def block_at(o, s):
        return out.at[o, s] if kind == "norm" else out.at[o, :, s]

    def gather_hop(way, h, s):
        at = block_at(there(way, place(way) - (h - 1)), s)
        src = obuf.at[s] if kind == "norm" and h == 1 else at
        return hop(way, n - 2 + h, s, src, at)

    def local_copy(s):
        src, dst = (obuf.at[s], out.at[z, s]) if kind == "norm" else (obuf.at[s, me], out.at[z, me, s])
        return pltpu.make_async_copy(src, dst, loc.at[s])

    def swap(r, s):
        return pltpu.make_async_remote_copy(src_ref=obuf.at[s, me ^ r], dst_ref=out.at[z, me, s], send_sem=a_send.at[r - 1, s], recv_sem=a_recv.at[r - 1, s], device_id=wd_to(r), device_id_type=MESH)

    def swapped(r, s):
        return pltpu.make_async_remote_copy(src_ref=obuf.at[s, me ^ r], dst_ref=out.at[z, me ^ r, s], send_sem=a_send.at[r - 1, s], recv_sem=a_recv.at[r - 1, s], device_id=wd_to(r), device_id_type=MESH)

    def weight_copy(q, j):
        i, p = q // PIECES, q % PIECES
        far_a, core, both_a, far_b, both_b = shipped[5 * i:5 * i + 5]
        size = ship[i].shape[0] // (2 * PIECES)
        own_at, at = pl.ds((PIECES * dp + p) * size, size), pl.ds(p * size, size)
        if j == 4:
            src, dst = ship[i], core
        elif j == 0:
            src, dst = ship[i].at[own_at], far_a.at[at]
        else:
            src, dst = ((far_a, far_b), (far_a, both_a), (far_b, both_b))[j - 1]
            src, dst = src.at[at], dst.at[at]
        to = (wd_to(2), {'dp': 1 - dp}, wd_to(1), wd_to(1), wd_to(1))[j]
        return pltpu.make_async_remote_copy(src_ref=src, dst_ref=dst, send_sem=w_send.at[q, j], recv_sem=w_recv.at[q, j], device_id=to, device_id_type=MESH)

    def row_places(pieces):
        own, core, far_a, far_b, both_a, both_b = pieces
        size, part_size = own.shape[0], far_a.shape[0]
        return ((own, 0), (core, size), (far_a, 2 * size + dp * part_size), (far_b, 2 * size + (1 - dp) * part_size), (both_a, 3 * size + dp * part_size), (both_b, 3 * size + (1 - dp) * part_size))

    def mix_copy(r, landed):
        there_at = mixbuf.at[me ^ r if landed else me, pl.ds(n - mixed.shape[1], mixed.shape[1])]
        return pltpu.make_async_remote_copy(src_ref=mixed.at[r], dst_ref=there_at, send_sem=a_send.at[r - 1], recv_sem=a_recv.at[r - 1], device_id=wd_to(r), device_id_type=MESH)

    def row_copy(r):
        return pltpu.make_async_remote_copy(src_ref=x_line.at[me ^ r], dst_ref=xbuf.at[r], send_sem=x_send.at[r - 1], recv_sem=x_recv.at[r - 1], device_id=wd_to(r), device_id_type=MESH)

    if kind == "norm":
        for r in OTHERS:
            mix_copy(r, False).start()
        for r in OTHERS:
            row_copy(r).start()
        jobs = [(x_line.at[me], xbuf.at[0]), (mixed.at[0], mixbuf.at[me, pl.ds(n - mixed.shape[1], mixed.shape[1])])]
        jobs += [(src, mixbuf.at[me ^ r, pl.ds(0, src.shape[0])]) for r, src in enumerate(mix_in)]
        jobs += [(w, wo.at[pl.ds(to, w.shape[0])]) for w, to in row_places(o_parts)]
        loads = [pltpu.make_async_copy(src, dst, pre_sem.at[j]) for j, (src, dst) in enumerate(jobs)]
        for copy in loads:
            copy.start()
        for q in range(PIECES * n_ship - 1):
            weight_copy(q, 0).start()
        for i in range(n_ship):
            weight_copy(PIECES * i, 4).start()

        def project(j, _):
            d, r = lax.div(j, 4), lax.rem(j, 4)
            depth = mixbuf.shape[3]
            acc = None
            for b in BLOCKS:
                at = pl.ds(pl.multiple_of((4 * r + b) * depth, depth), depth)
                val = dot32(mixbuf[b, d], wo[at, :])
                acc = val if acc is None else acc + val
            part[d, :, r] = acc.astype(BF16).reshape(steps, part.shape[3], part.shape[4])
            return 0

        for copy in loads:
            copy.wait()
        first = 4 * mix_in[0].shape[0]
        lax.fori_loop(0, first, project, 0)
        for r in OTHERS:
            mix_copy(r, True).wait_recv()
        lax.fori_loop(first, 4 * n, project, 0)

    crossed = PIECES * n_ship - PIECES // 2
    half = steps // 2
    if kind != "norm":
        gates = inner.shape[1] // TILE
        per_block = part.shape[4] // TILE
        tiles = gates + 4 * per_block
        loads = [pltpu.make_async_copy(m_all.at[:, pl.ds(i * half, half)], mbuf.at[i], pre_sem.at[i]) for i in WAYS]

        def tile_copies(q, down_block):
            slot = lax.rem(q, 2)
            if down_block is None:
                at = pl.ds(pl.multiple_of(q * TILE, TILE), TILE)
                jobs = [(w, i, to) for i, pieces in enumerate((g_parts, u_parts)) for w, to in row_places(pieces)]
            else:
                at = pl.ds(pl.multiple_of(lax.rem(q - gates, per_block) * TILE, TILE), TILE)
                own, core, far_a, far_b, both_a, both_b = d_parts
                rows_a = dp * (own.shape[0] // 2)
                rows_b = own.shape[0] // 2 - rows_a
                late, late_y = rows_b + far_b.shape[0], rows_a + far_a.shape[0]
                jobs = ([(own, 0, 0)], [(core, 0, 0)], [(far_a, 0, rows_a), (far_b, 0, rows_b), (late_b, 0, late), (late_a, 0, late_y)], [(both_a, 0, rows_a), (both_b, 0, rows_b), (late_both, 0, late), (late_both_a, 0, late_y)])[down_block]
            return [pltpu.make_async_copy(w.at[:, at], wbuf.at[slot, i, pl.ds(to, w.shape[0]), :], tile_sem.at[slot, j]) for j, (w, i, to) in enumerate(jobs)]

        def for_tile(q, act):
            @pl.when(q < gates)
            def _():
                for copy in tile_copies(q, None):
                    act(copy)

            for r in BLOCKS:
                @pl.when((q >= gates + r * per_block) & (q < gates + (r + 1) * per_block))
                def _(r=r):
                    for copy in tile_copies(q, r):
                        act(copy)

        def late_copy(j):
            size = late_a.shape[0]
            own, far_a = d_parts[0], d_parts[2]
            one, two = pl.ds(0, size), pl.ds(size, size)
            src, dst, to = (
                (far_a.at[pl.ds(far_a.shape[0] - size, size)], late_b.at[one], {'dp': 1 - dp}),
                (own.at[pl.ds((PIECES * dp + PIECES - 1) * size, size)], late_a, wd_to(2)),
                (late_a, late_b.at[two], {'dp': 1 - dp}),
                (late_a, late_both_a, wd_to(1)),
                (late_b.at[one], late_both.at[one], wd_to(1)),
                (late_b.at[two], late_both.at[two], wd_to(1)),
            )[j]
            return pltpu.make_async_remote_copy(src_ref=src, dst_ref=dst, send_sem=l_send.at[j], recv_sem=l_recv.at[j], device_id=to, device_id_type=MESH)

        late_copy(0).start()
        late_copy(1).start()

        def mlp_tile(job, _):
            phase, q = lax.div(job, tiles), lax.rem(job, tiles)

            @pl.when(job == gates // 2)
            def _():
                late_copy(1).wait_recv()
                late_copy(2).start()
                late_copy(3).start()

            @pl.when(job == gates + per_block)
            def _():
                late_copy(0).wait_recv()
                late_copy(4).start()
                late_copy(2).wait_recv()
                late_copy(5).start()

            @pl.when(job == gates + 3 * per_block - 1)
            def _():
                for j in OTHERS:
                    late_copy(j + 2).wait_recv()

            for_tile(q, lambda copy: copy.wait())

            @pl.when(job < 2 * tiles - 1)
            def _():
                for_tile(lax.rem(job + 1, tiles), lambda copy: copy.start())

            slot = lax.rem(q, 2)
            toks = inner.shape[0]

            @pl.when(q < gates)
            def _():
                at = pl.ds(pl.multiple_of(q * TILE, TILE), TILE)
                sums = []
                for i in range(2):
                    sums.append(dot32(mbuf[phase].reshape(toks, mbuf.shape[4]), wbuf[slot, i]))
                gate = jax.nn.gelu(sums[0] + bias_g[:, at], approximate=True)
                inner[:, at] = (gate * (sums[1] + bias_u[:, at])).astype(BF16)

            @pl.when(q >= gates)
            def _():
                d = q - gates
                at = pl.ds(pl.multiple_of(lax.rem(d, per_block) * TILE, TILE), TILE)
                val = dot32(inner[...], wbuf[slot, 0, 0:inner.shape[1], :]).astype(BF16)
                part[:, pl.ds(phase * half, half), lax.div(d, per_block), :, at] = val.reshape(n, half, part.shape[3], TILE)

            return 0

        for copy in loads:
            copy.start()
        for_tile(0 * z, lambda copy: copy.start())
        loads[0].wait()
        lax.fori_loop(0, tiles, mlp_tile, 0)
        loads[1].wait()

    def finish(s):
        for way in WAYS:
            p = place(way)

            @pl.when(p > 0)
            def _(way=way):
                reduce_wait(way, n - 1, s)

        total = 0.0
        for r in BLOCKS:
            val = part[z, s, r].astype(F32)
            val = val + jnp.where(z > 0, rbuf[0, n - 2, s, r].astype(F32), 0.0)
            val = val + jnp.where(z < n - 1, rbuf[1, n - 2, s, r].astype(F32), 0.0)
            if kind == "norm":
                val = xbuf[r, s].astype(F32) + val + bias[r]
                res_ref[s, r] = val
                total = total + jnp.sum(val * val, axis=1, keepdims=True)
            else:
                obuf[s, me ^ r] = (res_ref[s, r] + val + bias[r]).astype(BF16)
        if kind == "norm":
            width = res_ref.shape[3]
            scale = lax.rsqrt(total / (4 * width) + EPS)
            for r in BLOCKS:
                normed = (res_ref[s, r] * scale * (1.0 + gain[r])).astype(BF16)
                obuf[s, :, r * width:(r + 1) * width] = normed
        else:
            for r in OTHERS:
                swap(r, s).start()
        local_copy(s).start()

    def step(t, _):
        if kind == "norm":
            @pl.when(t == n - 1)
            def _():
                for r in OTHERS:
                    row_copy(r).wait_recv()

        for h in range(n, 0, -1):
            s = t - (n - 1) - lag - (h - 1)

            @pl.when((s >= 0) & (s < steps))
            def _(h=h, s=s):
                if h == 1 and kind != "norm":
                    for r in OTHERS:
                        swapped(r, s).wait_recv()
                    local_copy(s).wait()
                if h == 1 and kind == "norm":
                    finish(s)
                for way in WAYS:
                    p = place(way)
                    if h > 1:
                        @pl.when(p >= h - 1)
                        def _(way=way):
                            at = block_at(there(way, place(way) - (h - 1)), s)
                            hop(way, n - 3 + h, s, at, at).wait_recv()
                    if h < n:
                        @pl.when((p >= h - 1) & (p < n - 1))
                        def _(way=way):
                            gather_hop(way, h, s).start()

        if lag:
            s = t - (n - 1)

            @pl.when((s >= 0) & (s < steps))
            def _(s=s):
                finish(s)

        for h in range(n - 1, 0, -1):
            s = t - (h - 1)
            for way in WAYS:
                p = place(way)

                @pl.when((s >= 0) & (s < steps) & (p < h))
                def _(h=h, s=s, way=way, p=p):
                    if h > 1:
                        @pl.when(p > 0)
                        def _():
                            reduce_wait(way, h - 1, s)
                            mine = part[there(way, p + n - h), s].astype(F32)
                            rbuf[way, h - 2, s] = (rbuf[way, h - 2, s].astype(F32) + mine).astype(BF16)
                            reduce_hop(way, h, s, False).start()

                    @pl.when(p == 0)
                    def _():
                        reduce_hop(way, h, s, True).start()

        if kind != "norm":
            @pl.when(t < half)
            def _():
                lax.fori_loop(tiles + lax.div(t * tiles, half), tiles + lax.div((t + 1) * tiles, half), mlp_tile, 0)

        if kind == "norm":
            for q in range(PIECES * n_ship - 1):
                @pl.when(t == (3 * q + 8) // 2)
                def _(q=q):
                    weight_copy(q, 0).wait_recv()
                    if q < crossed:
                        weight_copy(q, 1).start()
                    weight_copy(q, 2).start()

                if q < crossed:
                    @pl.when(t == (3 * q + 12) // 2)
                    def _(q=q):
                        weight_copy(q, 1).wait_recv()
                        weight_copy(q, 3).start()
        return 0

    lax.fori_loop(0, steps + 2 * n - 2 + lag, step, 0)

    def drain(s, _):
        for way in WAYS:
            p = place(way)
            for h in range(1, n):
                @pl.when(p < h)
                def _(way=way, h=h):
                    reduce_hop(way, h, s, True).wait_send()

                @pl.when((p >= h - 1) & (p < n - 1))
                def _(way=way, h=h):
                    gather_hop(way, h, s).wait_send()
        if kind == "norm":
            local_copy(s).wait()
        else:
            for r in OTHERS:
                swap(r, s).wait_send()
        return 0

    if kind != "norm":
        for j in range(6):
            late_copy(j).wait_send()

    lax.fori_loop(0, steps, drain, 0)
    if kind == "norm":
        for q in range(PIECES * n_ship - 1):
            weight_copy(q, 0).wait_send()
            weight_copy(q, 2).wait()
            if q < crossed:
                weight_copy(q, 1).wait_send()
                weight_copy(q, 3).wait()
        for i in range(n_ship):
            weight_copy(PIECES * i, 4).wait()
        for r in OTHERS:
            mix_copy(r, False).wait_send()
            row_copy(r).wait_send()


VM = pl.BlockSpec(memory_space=pltpu.VMEM)
ANY = pl.BlockSpec(memory_space=pl.ANY)
DMA = pltpu.SemaphoreType.DMA


def line_scratch(n, steps, block, done):
    sems = (2, 2 * n - 2, steps)
    return [pltpu.VMEM((2, n - 1, steps) + block, BF16), pltpu.VMEM((steps,) + done, BF16), DMA(sems), DMA(sems), DMA((steps,))]


def residual_norm(n, x_line, bias, gain, mixed, mix_in, o_parts, ship):
    _, steps, rows, width = x_line.shape
    out_w = []
    for w in ship:
        less = 1 if w is ship[-1] else 0
        near, late = (jax.ShapeDtypeStruct((w.shape[0] // (2 * PIECES) * (PIECES - k), w.shape[1]), BF16) for k in (less, 2 * less))
        out_w += [near, jax.ShapeDtypeStruct(w.shape, BF16), near, late, late]
    done = (rows, 4 * width)
    far = [x_line, mixed, *mix_in, *o_parts, *ship]
    pieces = PIECES * len(ship)
    outs = pl.pallas_call(
        functools.partial(line_body, "norm", len(ship)),
        in_specs=[VM] * 2 + [ANY] * len(far),
        out_specs=[VM, ANY] + [ANY] * len(out_w),
        out_shape=[jax.ShapeDtypeStruct((steps, 4, rows, width), F32), jax.ShapeDtypeStruct((n, steps) + done, BF16)] + out_w,
        scratch_shapes=line_scratch(n, steps, (4, rows, width), done) + [
            DMA((pieces, 5)), DMA((pieces, 5)),
            pltpu.VMEM((n, steps, 4, rows, width), BF16),
            pltpu.VMEM((4, n) + mixed.shape[2:], BF16),
            pltpu.VMEM((4 * width, width), BF16),
            DMA((3,)), DMA((3,)), DMA((12,)),
            pltpu.VMEM(x_line.shape, BF16), DMA((3,)), DMA((3,)),
        ],
        compiler_params=pltpu.CompilerParams(collective_id=0, has_side_effects=True, vmem_limit_bytes=LIMIT),
        cost_estimate=WORK,
        name="residual_norm",
    )(bias, gain, *far)
    return outs[0], outs[1], [outs[2 + 5 * i:7 + 5 * i] for i in range(len(ship))]


def finish_rows(n, res, bias, m_all, bias_g, bias_u, pieces):
    steps, _, rows, width = res.shape
    half = steps // 2
    late = pieces[-1].shape[0] // 2
    inner_width = bias_g.shape[1]
    toks = n * half * rows
    return pl.pallas_call(
        functools.partial(line_body, "finish", 0),
        in_specs=[VM, VM, ANY, VM, VM] + [ANY] * len(pieces),
        out_specs=[ANY] * 5,
        out_shape=[jax.ShapeDtypeStruct((n, 4, steps, rows, width), BF16)] + [jax.ShapeDtypeStruct((late * k, pieces[-1].shape[1]), BF16) for k in (2, 2, 1, 1)],
        scratch_shapes=line_scratch(n, steps, (4, rows, width), (4, rows, width)) + [
            DMA((3, steps)), DMA((3, steps)),
            pltpu.VMEM((n, steps, 4, rows, width), BF16),
            pltpu.VMEM((2, n, half) + m_all.shape[2:], BF16),
            pltpu.VMEM((toks, inner_width), BF16),
            pltpu.VMEM((2, 2, 4 * width, TILE), BF16),
            DMA((2,)), DMA((2, 12)), DMA((6,)), DMA((6,)),
        ],
        compiler_params=pltpu.CompilerParams(collective_id=1, has_side_effects=True, vmem_limit_bytes=LIMIT),
        cost_estimate=WORK,
        name="finish_rows",
    )(res, bias, m_all, bias_g, bias_u, *pieces)[0]


def solution(mesh):
    wd_count = mesh.shape['wd']
    ch_count = mesh.shape['ch']
    row_spec = P('dp', 'wd')
    specs = (row_spec, P('dp'), P('wd'), P('wd', 'ch'), P('ch'), P('wd', 'ch'), P('ch'), P(None, 'ch'), P('ch'), P('ch'), P('ch'), P('ch'), P('ch'), P('ch'), P('ch', 'wd'), P('wd'), P('wd'), P('wd', 'ch'), P('ch'), P('wd', 'ch'), P('ch'), P('ch', 'wd'), P('wd'))
    core_hop, y_hop, both_hop = (flip_pairs(wd_count, r) for r in OTHERS)

    def local_layer(resid_in, seg_pos, gain_temporal, w_x, bias_x, w_y, bias_y, conv_w, conv_bias, lam_param, rgate_w, rgate_b, igate_w, igate_b, w_o, bias_o, gain_mlp, w_g, bias_g, w_u, bias_u, w_d, bias_d):
        me, z, dp = lax.axis_index('wd'), lax.axis_index('ch'), lax.axis_index('dp')
        idx = jnp.stack([me, dp, z]).astype(jnp.int32)
        tokens, local_width = resid_in.shape
        model_width = local_width * wd_count
        unit = tokens // sum(SPLIT)
        share = tokens // (ch_count * wd_count)
        rows = share // SUB
        channels = w_x.shape[1] // wd_count

        def half_from_y(w):
            half = w.shape[0] // 2
            part = lax.dynamic_slice_in_dim(w, dp * half, half, 0)
            return lax.ppermute(part, 'wd', y_hop)

        def gathered(w):
            far_a = half_from_y(w)
            far_b = lax.ppermute(far_a, 'dp', flip_pairs(2, 1))
            core = lax.ppermute(w, 'wd', core_hop)
            both_a = lax.ppermute(far_a, 'wd', core_hop)
            both_b = lax.ppermute(far_b, 'wd', core_hop)
            return w, core, far_a, far_b, both_a, both_b

        vecs = jnp.stack([bias_o, gain_mlp, bias_d])
        vecs = [vecs] + [lax.ppermute(vecs, 'wd', hop) for hop in (core_hop, y_hop, both_hop)]
        vecs = jnp.stack(vecs).astype(F32)[:, :, None, :]
        bias_o_r, gain_r, bias_d_r = vecs[:, 0], vecs[:, 1], vecs[:, 2]

        blocks = resid_in.reshape(ch_count, wd_count, share, local_width)
        line = lax.dynamic_index_in_dim(blocks, z, 0, keepdims=False)
        line = line.reshape(wd_count, SUB, rows, local_width)

        resid32 = resid_in.astype(F32)
        sum_sq = lax.psum(jnp.sum(resid32 * resid32, axis=1, keepdims=True), 'wd')
        normed = (resid32 * lax.rsqrt(sum_sq / model_width + EPS) * (1.0 + gain_temporal.astype(F32))).astype(BF16)

        cols = lambda arr, r: lax.dynamic_slice_in_dim(arr, (me ^ r) * channels, channels, arr.ndim - 1)
        wxy = [jnp.concatenate([cols(w_x, r), cols(w_y, r)], axis=1) for r in range(4)]
        w_send = jnp.concatenate([wxy[1], wxy[3]], axis=1)
        mine = lambda arr: cols(arr.astype(F32)[None], 0)
        bias_xy = jnp.concatenate([mine(bias_x), mine(bias_y)], axis=1)
        conv = jnp.concatenate([cols(conv_w.astype(F32), 0), mine(conv_bias), jnp.zeros((3, channels), F32)], axis=0)
        soft = jax.nn.softplus(-mine(lam_param))
        block = lambda arr: lax.dynamic_index_in_dim(arr, me, 0, keepdims=False)
        gate_w = jnp.concatenate([block(rgate_w), block(igate_w)], axis=1)
        gate_b = jnp.concatenate([mine(rgate_b), mine(igate_b)], axis=1)
        pos = seg_pos.reshape(tokens, 1)

        w_o_parts = gathered(w_o)

        tail = jnp.zeros((GROUP, channels), F32)
        carry = jnp.zeros((GROUP, channels), F32)
        for k, size in enumerate(SPLIT):
            start, stop = sum(SPLIT[:k]) * unit, sum(SPLIT[:k + 1]) * unit
            n = lax.slice_in_dim(normed, start, stop, axis=0)
            sent = dot32(n, w_send).astype(BF16)
            sent = lax.ppermute(sent, 'wd', core_hop)
            far = (dot32(n, wxy[2]) + sent[:, 2 * channels:].astype(F32)).astype(BF16)
            far = lax.ppermute(far, 'wd', y_hop)
            own = dot32(n, wxy[0]).astype(BF16)
            mixed, tail, carry = lru(idx, own, sent, far, pos[start:stop], bias_xy, conv, soft, gate_w, gate_b, tail, carry, share)
            if k == 0:
                mix_in = [mixed[0]] + [lax.ppermute(mixed[r], 'wd', hop) for r, hop in zip(OTHERS, (core_hop, y_hop, both_hop))]
        res, m, got = residual_norm(ch_count, line, bias_o_r, gain_r, mixed, mix_in, w_o_parts, [w_g, w_u, w_d])
        g_parts, u_parts, d_parts = ([w, core, far_a, far_b, both_a, both_b] for w, (far_a, core, both_a, far_b, both_b) in zip((w_g, w_u, w_d), got))
        bias_gu = [b.astype(F32)[None] for b in (bias_g, bias_u)]
        return finish_rows(ch_count, res, bias_d_r, m, *bias_gu, g_parts + u_parts + d_parts).reshape(tokens, local_width)

    return jax.shard_map(local_layer, mesh=mesh, in_specs=specs, out_specs=row_spec, check_vma=False)
```
